256 devices in a mesh: obs: 4 (over y), par: 64 (over x, z, core).
Axes of the slice: x: 4, y: 4, z: 8, core: 2. Of those that a mesh axis runs over, the one named last changes fastest.
Arguments:
- jacobian: bfloat16 [2048, 262144], P('obs', 'par'), may hold values from -0.01171875 to 0.01171875
- probes: bfloat16 [262144, 256], P('par'), may hold values from -6 to 6
- coeffs: bfloat16 [2048, 3, 128, 128], P('par'), may hold values from -0.3125 to 0.3125
- offsets: int32 [2048, 2], P('par'), may hold values from -4 to 4
Outputs:
- ritz_basis: bfloat16 [262144, 256], P('par')
- basis_image: bfloat16 [262144, 256], P('par')
- ritz_matrix: float32 [256, 256], replicated
The draws below stay inside these ranges and needn't reach their ends.
All inputs are finite; a program needn't handle non-finite values.
Results may differ from the reference program's by a relative error of at most 0.015.
Values may be sent and summed in bfloat16 or wider, within the bound.
No kernel may reach another device: no remote copies, remote signals or barrier semaphores. Data moves between devices by JAX's collectives and lax.ppermute only.
A program may use at most 128 MiB of HBM per device.

```python
import jax
import jax.numpy as jnp
from jax import lax

OBS_DEV = 512
K = 256
BLK = 128
REACH = 4
NOBS = 2048
NPAR = 262144
NBLK = 2048
N_OBS = 4


def set_ends(values, rng, smallest, high):
    index_at = [jax.random.randint(jax.random.fold_in(rng, axis), (), 0, length) for axis, length in enumerate(values.shape)]
    longest = values.shape.index(max(values.shape))
    beside = index_at[:longest] + [(index_at[longest] + 1) % values.shape[longest]] + index_at[longest + 1:]
    return values.at[tuple(index_at)].set(smallest).at[tuple(beside)].set(high)


def block_levels(rng, shape, shards, smallest, high):
    gain, own = 1.0, jax.random.fold_in(rng, 6)
    for position, blocks in shards:
        steps = jnp.exp(jax.random.uniform(jax.random.fold_in(own, position), (blocks,), jnp.float32, smallest / len(shards), high / len(shards)))
        gain = gain * jnp.repeat(steps, shape[position] // blocks).reshape([-1 if axis == position else 1 for axis in range(len(shape))])
    return gain


def normal_values(key, extent, deviation, bound, split=(), held_as=jnp.bfloat16):
    entries = jax.random.normal(key, extent, jnp.float32) * deviation
    if len(split) > 0:
        entries = block_levels(key, extent, split, -0.22, 0.18) * entries
    return jnp.clip(entries, min=-bound, max=bound).astype(held_as)


def setup_inputs(seed: int = 0) -> dict:
    keys = jax.random.split(jax.random.key(seed), 5)
    jacobian = normal_values(keys[0], (NOBS, NPAR), NPAR ** -0.5, 0.01171875, ((0, 4), (1, 64)))
    probes = normal_values(keys[1], (NPAR, K), 1.0, 6.0, ((0, 64),))
    coeffs = normal_values(keys[2], (NBLK, 3, BLK, BLK), (3 * BLK) ** -0.5, 0.3125, ((0, 64),))
    offsets = set_ends(jax.random.randint(keys[3], (NBLK, 2), -REACH, REACH + 1), jax.random.fold_in(keys[3], 1), -REACH, REACH).astype(jnp.int32)
    return dict(jacobian=jacobian, probes=probes, coeffs=coeffs, offsets=offsets)


def block_index(offsets):
    count = offsets.shape[0]
    full_offsets = jnp.concatenate([jnp.zeros((count, 1), jnp.int32), offsets.astype(jnp.int32)], axis=1)
    return (jnp.arange(count, dtype=jnp.int32)[:, None] + REACH + full_offsets).astype(jnp.int32)

def prior_forward(values, coeffs, offsets):
    width = values.shape[1]
    positions = block_index(offsets)
    padded = jnp.pad(values, ((REACH * BLK, REACH * BLK), (0, 0))).reshape(-1, BLK, width)
    picked = padded[positions]
    result = jnp.einsum('bjrc,bjcn->brn', coeffs.astype(jnp.float32), picked.astype(jnp.float32))
    return result.reshape(-1, width).astype(jnp.bfloat16)

def prior_adjoint(values, coeffs, offsets):
    width = values.shape[1]
    count = offsets.shape[0]
    positions = block_index(offsets)
    blocks = values.reshape(count, BLK, width)
    contrib = jnp.einsum('bjcr,bcn->bjrn', coeffs.astype(jnp.float32), blocks.astype(jnp.float32))
    accumulated = jnp.zeros((count + 2 * REACH, BLK, width), jnp.float32).at[positions].add(contrib)
    return accumulated[REACH:REACH + count].reshape(-1, width)

def reference(jacobian, probes, coeffs, offsets):
    sampled = prior_forward(probes, coeffs, offsets)
    forward = jnp.dot(jacobian.astype(jnp.float32), sampled.astype(jnp.float32), preferred_element_type=jnp.float32).astype(jnp.bfloat16)
    adjoint_total = jnp.zeros((NPAR, K), jnp.float32)
    for shard in range(N_OBS):
        jac_rows = jacobian[shard * OBS_DEV:(shard + 1) * OBS_DEV]
        fwd_rows = forward[shard * OBS_DEV:(shard + 1) * OBS_DEV]
        partial_sum = lax.dot_general(jac_rows.astype(jnp.float32), fwd_rows.astype(jnp.float32), (((0,), (0,)), ((), ())), preferred_element_type=jnp.float32)
        rounded = lax.optimization_barrier(partial_sum.astype(jnp.bfloat16))
        adjoint_total = adjoint_total + rounded.astype(jnp.float32)
    adjoint = adjoint_total.astype(jnp.bfloat16)
    range_sample = prior_adjoint(adjoint, coeffs, offsets)
    gram_matrix = jnp.dot(range_sample.T, range_sample, precision=lax.Precision.HIGHEST) / NPAR
    lower_factor = jnp.linalg.cholesky(gram_matrix)
    solved = lax.linalg.triangular_solve(lower_factor, range_sample, left_side=False, lower=True, transpose_a=True)
    ritz_basis = solved.astype(jnp.bfloat16)
    basis_image = prior_forward(ritz_basis, coeffs, offsets)
    projected = jnp.dot(jacobian.astype(jnp.float32), basis_image.astype(jnp.float32), preferred_element_type=jnp.float32)
    ritz_matrix = jnp.dot(projected.T, projected, precision=lax.Precision.HIGHEST) / NOBS
    return (ritz_basis, basis_image, ritz_matrix)
```

```python
import functools

import jax
import jax.numpy as jnp
from jax import lax
from jax.experimental import pallas as pl
from jax.experimental.pallas import tpu as pltpu
from jax.sharding import PartitionSpec as P

BLK = 128
REACH = 4
EDGE = REACH * BLK
NB = 64
F32 = jnp.float32
BF16 = jnp.bfloat16
HI = lax.Precision.HIGHEST
VMEM = pl.BlockSpec(memory_space=pltpu.VMEM)
SMEM = pl.BlockSpec(memory_space=pltpu.SMEM)


def call(kernel, name, outs, specs, args, scratch=(), mib=24, flops=0):
    return pl.pallas_call(
        kernel,
        name=name,
        out_shape=outs,
        in_specs=specs,
        out_specs=jax.tree.map(lambda _: VMEM, outs),
        scratch_shapes=scratch,
        compiler_params=pltpu.CompilerParams(vmem_limit_bytes=mib * 2**20),
        cost_estimate=pl.CostEstimate(flops=flops, bytes_accessed=0, transcendentals=0),
    )(*args)


def dot(a, b):
    return jnp.dot(a, b, preferred_element_type=F32)


def dot_tn(a, b, precision=None):
    return lax.dot_general(a, b, (((0,), (0,)), ((), ())), precision=precision, preferred_element_type=F32)


def dot_nt(a, b, precision=None):
    return lax.dot_general(a, b, (((1,), (1,)), ((), ())), precision=precision, preferred_element_type=F32)


def shape(*dims, dtype=BF16):
    return jax.ShapeDtypeStruct(dims, dtype)


def edges_kernel(off_ref, jac_ref, coef_ref, low_ref, high_ref, acc):
    count = coef_ref.shape[0]
    acc[...] = jnp.zeros_like(acc)
    for side, first in ((0, 0), (1, count - REACH)):
        for i in range(REACH):
            block = first + i
            columns = jac_ref[:, block * BLK : (block + 1) * BLK]
            for j in range(2):
                target = block + off_ref[block, j]
                place = target + REACH if side == 0 else target - count + REACH
                outside = target < 0 if side == 0 else target >= count

                @pl.when(outside)
                def _():
                    acc[place] += dot(columns, coef_ref[block, j + 1])

    for i in range(REACH):
        low_ref[:, i * BLK : (i + 1) * BLK] = acc[i].astype(BF16)
        high_ref[:, i * BLK : (i + 1) * BLK] = acc[i + REACH].astype(BF16)


def own_kernel(off_ref, jac_ref, coef_ref, out_ref, acc):
    count = coef_ref.shape[0]

    def diagonal(block, carry):
        columns = jac_ref[:, pl.ds(pl.multiple_of(block * BLK, BLK), BLK)]
        acc[block] = dot(columns, coef_ref[block, 0])
        return carry

    lax.fori_loop(0, count, diagonal, 0, unroll=2)

    def band(block, carry):
        columns = jac_ref[:, pl.ds(pl.multiple_of(block * BLK, BLK), BLK)]
        both = jnp.concatenate([coef_ref[block, 1], coef_ref[block, 2]], axis=1)
        terms = dot(columns, both)
        for j in range(2):
            target = block + off_ref[block, j]

            @pl.when((target >= 0) & (target < count))
            def _():
                acc[target] += terms[:, j * BLK : (j + 1) * BLK]

        return carry

    lax.fori_loop(0, count, band, 0)
    for block in range(count):
        out_ref[:, block * BLK : (block + 1) * BLK] = acc[block].astype(BF16)


def forward_kernel(own_ref, left_ref, right_ref, probe_ref, full_ref, part_ref):
    width = own_ref.shape[1]
    first = (own_ref[:, :EDGE].astype(F32) + left_ref[...].astype(F32)).astype(BF16)
    last = (own_ref[:, width - EDGE :].astype(F32) + right_ref[...].astype(F32)).astype(BF16)
    full_ref[:, :EDGE] = first
    full_ref[:, EDGE : width - EDGE] = own_ref[:, EDGE : width - EDGE]
    full_ref[:, width - EDGE :] = last
    part_ref[...] = dot(full_ref[...], probe_ref[...]).astype(BF16)


def total_kernel(parts_ref, out_ref):
    total = parts_ref[0].astype(F32)
    for i in range(1, parts_ref.shape[0]):
        total += parts_ref[i].astype(F32)
    total = total.astype(BF16)
    for i in range(out_ref.shape[0]):
        out_ref[i] = total


def sample_kernel(ranks, me_ref, full_ref, fwd_ref, *outs):
    rows = full_ref.shape[1] // ranks // 2
    fwd = fwd_ref[...]
    for rel in range(ranks):
        owner = lax.rem(me_ref[0] + rel, ranks)
        for half in range(2):
            start = pl.multiple_of(owner * (2 * rows) + half * rows, rows)
            outs[2 * rel + half][...] = dot_tn(full_ref[:, pl.ds(start, rows)], fwd).astype(BF16)


def project_kernel(ranks, me_ref, full_ref, *refs):
    pieces, (sample_ref, part_ref, low_ref, high_ref) = refs[: 2 * ranks], refs[2 * ranks :]
    rows = pieces[0].shape[0]
    total = jnp.zeros(part_ref.shape, F32)
    for rel in range(ranks):
        owner = lax.rem(me_ref[0] + rel, ranks)
        for half in range(2):
            piece = pieces[2 * rel + half][...]
            start = pl.multiple_of(owner * (2 * rows) + half * rows, rows)
            sample_ref[pl.ds(start, rows), :] = piece
            total += dot(full_ref[:, pl.ds(start, rows)], piece)
    part_ref[...] = total.astype(BF16)
    low_ref[...] = sample_ref[:EDGE, :]
    high_ref[...] = sample_ref[sample_ref.shape[0] - EDGE :, :]


def prior_kernel(off_ref, coef_ref, sample_ref, below_ref, above_ref, out_ref, ext):
    count, rows = coef_ref.shape[0], sample_ref.shape[0]
    ext[:EDGE] = below_ref[...]
    ext[EDGE : EDGE + rows] = sample_ref[...]
    ext[EDGE + rows :] = above_ref[...]

    def apply(block, carry):
        picked = [ext[pl.ds(pl.multiple_of((block + REACH) * BLK, BLK), BLK), :]]
        for j in range(2):
            start = (block + REACH + off_ref[block, j]) * BLK
            picked.append(ext[pl.ds(pl.multiple_of(start, BLK), BLK), :])
        wide = jnp.concatenate([coef_ref[block, j] for j in range(3)], axis=1)
        result = dot(wide, jnp.concatenate(picked, axis=0))
        out_ref[pl.ds(pl.multiple_of(block * BLK, BLK), BLK), :] = result.astype(BF16)
        return carry

    lax.fori_loop(0, count, apply, 0, unroll=2)


def packed(full):
    half = full.shape[0] // 2
    return jnp.concatenate([full[:half, :half], full[:half, half:], full[half:, half:]], axis=0)


def moments_kernel(fwd_ref, proj_ref, gram_ref, second_ref):
    proj = proj_ref[...]
    gram = dot_tn(fwd_ref[...], proj)
    gram_ref[...] = packed(0.5 * (gram + gram.T))
    second_ref[...] = packed(dot_tn(proj, proj)).astype(BF16)


def row_of(tile, k):
    return jnp.broadcast_to(tile[k : k + 1, :], tile.shape)


def lane_of(tile, k):
    return jnp.broadcast_to(tile[:, k : k + 1], (8, 2 * NB))


def factor_inverse(block):
    index = [lax.broadcasted_iota(jnp.int32, (NB, NB), d) for d in (0, 1)]
    wide = jnp.concatenate([block, (index[0] == index[1]).astype(F32)], axis=1)
    groups = NB // 8
    tiles = [wide[8 * t : 8 * t + 8] for t in range(groups)]
    row = lax.broadcasted_iota(jnp.int32, (8, 2 * NB), 0)
    out = []
    for g in range(groups):
        cols = {t: [lane_of(tiles[t], 8 * g + k) for k in range(8)] for t in range(g, groups)}
        scale = jnp.ones((8, 2 * NB), F32)
        for k in range(8):
            pivot = row_of(cols[g][k], k)
            inverse = 1.0 / pivot
            scale = jnp.where(row == k, lax.rsqrt(pivot), scale)
            pivot_row = row_of(tiles[g], k)
            heads = [row_of(cols[g][j], k) for j in range(k + 1, 8)]
            for t in range(g, groups):
                ratio = cols[t][k] * inverse
                if t == g:
                    ratio = jnp.where(row > k, ratio, 0.0)
                tiles[t] = tiles[t] - ratio * pivot_row
                for j in range(k + 1, 8):
                    cols[t][j] = cols[t][j] - ratio * heads[j - k - 1]
        out.append(tiles[g] * scale)
    return jnp.concatenate(out, axis=0)[:, NB:]


def factor_kernel(scale, *refs):
    parts, (out_ref, a_ref, m_ref) = refs[:-3], refs[-3:]
    n = out_ref.shape[0]
    half = n // 2
    total = parts[0][...]
    for part in parts[1:]:
        total += part[...]
    total *= scale
    a_ref[...] = jnp.zeros((n, n), F32)
    a_ref[:half, :half] = total[:half]
    a_ref[:half, half:] = total[half:n]
    a_ref[half:, half:] = total[n:]
    m_ref[...] = jnp.zeros((n, n), F32)
    out_ref[...] = jnp.zeros((n, n), F32)
    for lo in range(0, n, NB):
        hi = lo + NB
        inverse = factor_inverse(a_ref[lo:hi, lo:hi])
        out_ref[lo:hi, lo:hi] = inverse
        if lo:
            out_ref[lo:hi, :lo] = jnp.dot(inverse, m_ref[lo:hi, :lo], precision=HI, preferred_element_type=F32)
        if hi < n:
            upper = jnp.dot(inverse, a_ref[lo:hi, hi:], precision=HI, preferred_element_type=F32)
            a_ref[hi:, hi:] -= dot_tn(upper, upper, HI)
            m_ref[hi:, :hi] -= dot_tn(upper, out_ref[lo:hi, :hi], HI)


def final_kernel(scale, inv_ref, sample_ref, image_ref, *refs):
    seconds, (basis_ref, mapped_ref, ritz_ref) = refs[:-3], refs[-3:]
    inverse = inv_ref[...]
    low = inverse.astype(BF16)
    basis_ref[...] = dot_nt(sample_ref[...], low).astype(BF16)
    mapped_ref[...] = dot_nt(image_ref[...], low).astype(BF16)

    @pl.when(pl.program_id(0) == 0)
    def _():
        n = inverse.shape[0]
        half = n // 2
        total = seconds[0][...].astype(F32)
        for part in seconds[1:]:
            total += part[...].astype(F32)
        upper = total[half:n]
        full = jnp.concatenate(
            [
                jnp.concatenate([total[:half], upper], axis=1),
                jnp.concatenate([upper.T, total[n:]], axis=1),
            ],
            axis=0,
        )
        left = jnp.dot(inverse, full, precision=HI, preferred_element_type=F32)
        ritz_ref[...] = dot_nt(left, inverse, HI) * scale


def shifted(value, axis, by, wrap=True):
    count = lax.axis_size(axis)
    pairs = [(i, (i + by) % count) for i in range(count) if wrap or 0 <= i + by < count]
    return lax.ppermute(value, axis, pairs)


def added(*values):
    return sum(v.astype(F32) for v in values).astype(BF16)


def summed_over_par(part):
    rows, width = part.shape
    count = lax.axis_size("par")
    parts = lax.all_to_all(part.reshape(count, rows // count, width), "par", 0, 0, tiled=True)
    own = call(total_kernel, "total", shape(*parts.shape), [VMEM], [parts], mib=4)
    return lax.all_to_all(own, "par", 0, 0, tiled=True).reshape(rows, width)


def body(jacobian, probes, coeffs, offsets):
    ranks = lax.axis_size("obs")
    nobs, npar = jacobian.shape[0], jacobian.shape[1]
    width = probes.shape[1]
    count = coeffs.shape[0]
    me = lax.axis_index("obs").reshape(1)
    flops = 2 * nobs * npar * width

    low, high = call(
        edges_kernel,
        "edges",
        [shape(nobs, EDGE)] * 2,
        [SMEM, VMEM, VMEM],
        [offsets, jacobian, coeffs],
        [pltpu.VMEM((2 * REACH, nobs, BLK), F32)],
        flops=flops // 4,
    )
    from_left = shifted(high, "par", 1, False)
    from_right = shifted(low, "par", -1, False)
    own = call(
        own_kernel,
        "own",
        shape(nobs, npar),
        [SMEM, VMEM, VMEM],
        [offsets, jacobian, coeffs],
        [pltpu.VMEM((count, nobs, BLK), F32)],
        flops=4 * flops,
    )
    full, part = call(
        forward_kernel,
        "forward",
        [shape(nobs, npar), shape(nobs, width)],
        [VMEM] * 4,
        [own, from_left, from_right, probes],
        flops=flops,
    )
    forward = summed_over_par(part)

    pieces = call(
        functools.partial(sample_kernel, ranks),
        "sample",
        [shape(npar // ranks // 2, width)] * (2 * ranks),
        [SMEM, VMEM, VMEM],
        [me, full, forward],
        flops=flops,
    )
    here0, here1, right0, right1, far0, far1, left0, left1 = pieces
    via_left = shifted(far0, "obs", 1)
    via_right = shifted(far1, "obs", -1)
    a1 = shifted(right1, "obs", 1)
    b0 = shifted(left0, "obs", -1)
    a0 = shifted(added(right0, via_left), "obs", 1)
    b1 = shifted(added(left1, via_right), "obs", -1)
    sum0 = added(here0, a0, b0)
    sum1 = added(here1, a1, b1)

    l0 = shifted(sum0, "obs", 1)
    r1 = shifted(sum1, "obs", -1)
    l1 = shifted(sum1, "obs", 1)
    r0 = shifted(sum0, "obs", -1)
    f0 = shifted(l0, "obs", 1)
    f1 = shifted(r1, "obs", -1)

    sample, part2, tail_low, tail_high = call(
        functools.partial(project_kernel, ranks),
        "project",
        [shape(npar, width), shape(nobs, width), shape(EDGE, width), shape(EDGE, width)],
        [SMEM] + [VMEM] * (1 + 2 * ranks),
        [me, full, sum0, sum1, r0, r1, f0, f1, l0, l1],
        flops=flops,
    )
    below = shifted(tail_high, "par", 1, False)
    above = shifted(tail_low, "par", -1, False)
    projected = summed_over_par(part2)
    image = call(
        prior_kernel,
        "prior",
        shape(npar, width),
        [SMEM] + [VMEM] * 4,
        [offsets, coeffs, sample, below, above],
        [pltpu.VMEM((npar + 2 * EDGE, width), BF16)],
        flops=flops,
    )

    gram, second = call(
        moments_kernel,
        "moments",
        [shape(3 * width // 2, width // 2, dtype=F32), shape(3 * width // 2, width // 2)],
        [VMEM] * 2,
        [forward, projected],
        mib=8,
        flops=flops // 8,
    )
    grams = [gram] + [shifted(gram, "obs", by) for by in (1, -1, 2)]
    seconds = [second] + [shifted(second, "obs", by) for by in (1, -1, 2)]
    total_par = npar * lax.axis_size("par")
    total_obs = nobs * ranks
    inverse = call(
        functools.partial(factor_kernel, 1.0 / total_par),
        "factor",
        shape(width, width, dtype=F32),
        [VMEM] * len(grams),
        grams,
        [pltpu.VMEM((width, width), F32)] * 2,
        mib=8,
        flops=16 * flops,
    )
    steps = 4
    rows = npar // steps
    whole = lambda *dims: pl.BlockSpec(dims, lambda i: (0,) * len(dims))
    by_rows = pl.BlockSpec((rows, width), lambda i: (i, 0))
    return pl.pallas_call(
        functools.partial(final_kernel, 1.0 / total_obs),
        name="final",
        grid=(steps,),
        out_shape=[shape(npar, width), shape(npar, width), shape(width, width, dtype=F32)],
        in_specs=[whole(width, width), by_rows, by_rows] + [whole(*second.shape)] * len(seconds),
        out_specs=[by_rows, by_rows, whole(width, width)],
        compiler_params=pltpu.CompilerParams(vmem_limit_bytes=16 * 2**20),
    )(inverse, sample, image, *seconds)


def solution(mesh):
    return jax.shard_map(
        body,
        mesh=mesh,
        in_specs=(P("obs", "par"), P("par", None), P("par", None, None, None), P("par", None)),
        out_specs=(P("par", None), P("par", None), P()),
        check_vma=False,
    )
```

```python
import functools

import jax
import jax.numpy as jnp
from jax import lax
from jax.experimental import pallas as pl
from jax.experimental.pallas import tpu as pltpu
from jax.sharding import PartitionSpec as P

BLK = 128
REACH = 4
EDGE = REACH * BLK
NB = 64
F32 = jnp.float32
BF16 = jnp.bfloat16
HI = lax.Precision.HIGHEST
VMEM = pl.BlockSpec(memory_space=pltpu.VMEM)
SMEM = pl.BlockSpec(memory_space=pltpu.SMEM)


def call(kernel, name, outs, specs, args, scratch=(), mib=24, flops=0):
    return pl.pallas_call(
        kernel,
        name=name,
        out_shape=outs,
        in_specs=specs,
        out_specs=jax.tree.map(lambda _: VMEM, outs),
        scratch_shapes=scratch,
        compiler_params=pltpu.CompilerParams(vmem_limit_bytes=mib * 2**20),
        cost_estimate=pl.CostEstimate(flops=flops, bytes_accessed=0, transcendentals=0),
    )(*args)


def dot(a, b):
    return jnp.dot(a, b, preferred_element_type=F32)


def dot_tn(a, b, precision=None):
    return lax.dot_general(a, b, (((0,), (0,)), ((), ())), precision=precision, preferred_element_type=F32)


def dot_nt(a, b, precision=None):
    return lax.dot_general(a, b, (((1,), (1,)), ((), ())), precision=precision, preferred_element_type=F32)


def shape(*dims, dtype=BF16):
    return jax.ShapeDtypeStruct(dims, dtype)


def edges_kernel(count, off_ref, jac_low, jac_high, coef_low, coef_high, low_ref, high_ref, acc):
    acc[...] = jnp.zeros_like(acc)
    for side, (jac, coef) in enumerate(((jac_low, coef_low), (jac_high, coef_high))):
        for i in range(REACH):
            block = i + side * (count - REACH)
            columns = jac[:, i * BLK : (i + 1) * BLK]
            for j in range(2):
                target = block + off_ref[j, block]
                place = target + REACH if side == 0 else target - count + REACH
                outside = target < 0 if side == 0 else target >= count

                @pl.when(outside)
                def _():
                    acc[place] += dot(columns, coef[i, j + 1])

    for i in range(REACH):
        low_ref[:, i * BLK : (i + 1) * BLK] = acc[i].astype(BF16)
        high_ref[:, i * BLK : (i + 1) * BLK] = acc[i + REACH].astype(BF16)


def own_kernel(off_ref, jac_ref, coef_ref, out_ref, acc):
    count = coef_ref.shape[0]
    for i in range(REACH):
        acc[i] = jnp.zeros_like(acc[i])
        acc[count + REACH + i] = jnp.zeros_like(acc[i])

    def diagonal(block, carry):
        columns = jac_ref[:, pl.ds(pl.multiple_of(block * BLK, BLK), BLK)]
        acc[block + REACH] = dot(columns, coef_ref[block, 0])
        return carry

    lax.fori_loop(0, count, diagonal, 0, unroll=4)

    def band(block, carry):
        columns = jac_ref[:, pl.ds(pl.multiple_of(block * BLK, BLK), BLK)]
        for j in range(2):
            acc[block + REACH + off_ref[j, block]] += dot(columns, coef_ref[block, j + 1])
        return carry

    lax.fori_loop(0, count, band, 0, unroll=4)
    for block in range(count):
        out_ref[:, block * BLK : (block + 1) * BLK] = acc[block + REACH].astype(BF16)


def forward_kernel(me_ref, own_ref, left_ref, right_ref, probe_ref, full_ref, keep_ref, give_ref):
    width = own_ref.shape[1]
    first = (own_ref[:, :EDGE].astype(F32) + left_ref[...].astype(F32)).astype(BF16)
    last = (own_ref[:, width - EDGE :].astype(F32) + right_ref[...].astype(F32)).astype(BF16)
    full_ref[:, :EDGE] = first
    full_ref[:, EDGE : width - EDGE] = own_ref[:, EDGE : width - EDGE]
    full_ref[:, width - EDGE :] = last
    rows = keep_ref.shape[0]
    core = me_ref[1]
    keep_ref[...] = dot(full_ref[pl.ds(pl.multiple_of(core * rows, rows), rows), :], probe_ref[...]).astype(BF16)
    give_ref[...] = dot(full_ref[pl.ds(pl.multiple_of((1 - core) * rows, rows), rows), :], probe_ref[...]).astype(BF16)


def pair_kernel(keep_ref, come_ref, out_ref):
    out_ref[...] = (keep_ref[...].astype(F32) + come_ref[...].astype(F32)).astype(BF16)


def total_kernel(parts_ref, out_ref):
    total = parts_ref[0].astype(F32)
    for i in range(1, parts_ref.shape[0]):
        total += parts_ref[i].astype(F32)
    total = total.astype(BF16)
    for i in range(out_ref.shape[0]):
        out_ref[i] = total


def in_order(me_ref, mine_ref, other_ref, out):
    rows = mine_ref.shape[0]
    out[pl.ds(pl.multiple_of(me_ref[1] * rows, rows), rows), :] = mine_ref[...]
    out[pl.ds(pl.multiple_of((1 - me_ref[1]) * rows, rows), rows), :] = other_ref[...]


def sample_kernel(ranks, me_ref, full_ref, mine_ref, other_ref, *refs):
    outs, fwd = refs[:-1], refs[-1]
    rows = full_ref.shape[1] // ranks // 2
    in_order(me_ref, mine_ref, other_ref, fwd)
    for rel in range(ranks):
        owner = lax.rem(me_ref[0] + rel, ranks)
        for half in range(2):
            start = pl.multiple_of(owner * (2 * rows) + half * rows, rows)
            outs[2 * rel + half][...] = dot_tn(full_ref[:, pl.ds(start, rows)], fwd[...]).astype(BF16)


def project_kernel(ranks, me_ref, full_ref, *refs):
    pieces = refs[: 2 * ranks]
    sample_ref, low_ref, high_ref, keep_ref, give_ref, acc = refs[2 * ranks :]
    rows = pieces[0].shape[0]
    total = jnp.zeros(acc.shape, F32)
    for rel in range(ranks):
        owner = lax.rem(me_ref[0] + rel, ranks)
        for half in range(2):
            piece = pieces[2 * rel + half][...]
            start = pl.multiple_of(owner * (2 * rows) + half * rows, rows)
            sample_ref[pl.ds(start, rows), :] = piece
            total += dot(full_ref[:, pl.ds(start, rows)], piece)
    acc[...] = total
    rows = keep_ref.shape[0]
    core = me_ref[1]
    keep_ref[...] = acc[pl.ds(pl.multiple_of(core * rows, rows), rows), :].astype(BF16)
    give_ref[...] = acc[pl.ds(pl.multiple_of((1 - core) * rows, rows), rows), :].astype(BF16)
    low_ref[...] = sample_ref[:EDGE, :]
    high_ref[...] = sample_ref[sample_ref.shape[0] - EDGE :, :]


def prior_kernel(off_ref, coef_ref, sample_ref, below_ref, above_ref, out_ref, ext):
    count, rows = coef_ref.shape[0], sample_ref.shape[0]
    ext[:EDGE] = below_ref[...]
    ext[EDGE : EDGE + rows] = sample_ref[...]
    ext[EDGE + rows :] = above_ref[...]

    def apply(block, carry):
        starts = [(block + REACH) * BLK] + [(block + REACH + off_ref[j, block]) * BLK for j in range(2)]
        result = sum(dot(coef_ref[block, j], ext[pl.ds(pl.multiple_of(starts[j], BLK), BLK), :]) for j in range(3))
        out_ref[pl.ds(pl.multiple_of(block * BLK, BLK), BLK), :] = result.astype(BF16)
        return carry

    lax.fori_loop(0, count, apply, 0, unroll=4)


def packed(full):
    return jnp.concatenate(
        [
            full[:NB, : 2 * NB],
            full[:NB, 2 * NB :],
            full[NB : 2 * NB, NB : 3 * NB],
            full[2 * NB : 3 * NB, 2 * NB :],
            jnp.concatenate([full[NB : 2 * NB, 3 * NB :], full[3 * NB :, 3 * NB :]], axis=1),
        ],
        axis=0,
    )


def unpacked(pack):
    r = [pack[i * NB : (i + 1) * NB] for i in range(5)]
    zero = jnp.zeros((NB, NB), F32)
    join = lambda *p: jnp.concatenate(p, axis=1)
    return jnp.concatenate(
        [join(r[0], r[1]), join(zero, r[2], r[4][:, :NB]), join(zero, zero, r[3]), join(zero, zero, zero, r[4][:, NB:])],
        axis=0,
    )


def moments_kernel(me_ref, fwd_mine, fwd_other, proj_mine, proj_other, out_ref, fwd, proj):
    in_order(me_ref, fwd_mine, fwd_other, fwd)
    in_order(me_ref, proj_mine, proj_other, proj)
    gram = dot_tn(fwd[...], proj[...])
    gram = packed(0.5 * (gram + gram.T))
    rows = gram.shape[0]
    high = gram.astype(BF16)
    out_ref[:rows] = high
    out_ref[rows : 2 * rows] = (gram - high.astype(F32)).astype(BF16)
    out_ref[2 * rows :] = packed(dot_tn(proj[...], proj[...])).astype(BF16)


def row_of(tile, k):
    return jnp.broadcast_to(tile[k : k + 1, :], tile.shape)


def lane_of(tile, k):
    return jnp.broadcast_to(tile[:, k : k + 1], (8, 2 * NB))


def factor_inverse(block):
    index = [lax.broadcasted_iota(jnp.int32, (NB, NB), d) for d in (0, 1)]
    wide = jnp.concatenate([block, (index[0] == index[1]).astype(F32)], axis=1)
    groups = NB // 8
    tiles = [wide[8 * t : 8 * t + 8] for t in range(groups)]
    row = lax.broadcasted_iota(jnp.int32, (8, 2 * NB), 0)
    out = []
    for g in range(groups):
        cols = {t: [lane_of(tiles[t], 8 * g + k) for k in range(8)] for t in range(g, groups)}
        scale = jnp.ones((8, 2 * NB), F32)
        for k in range(8):
            root = lax.rsqrt(row_of(cols[g][k], k))
            inverse = root * root
            scale = jnp.where(row == k, root, scale)
            pivot_row = row_of(tiles[g], k)
            heads = [row_of(cols[g][j], k) for j in range(k + 1, 8)]
            for t in range(g, groups):
                ratio = cols[t][k] * inverse
                if t == g:
                    ratio = jnp.where(row > k, ratio, 0.0)
                tiles[t] = tiles[t] - ratio * pivot_row
                for j in range(k + 1, 8):
                    cols[t][j] = cols[t][j] - ratio * heads[j - k - 1]
        out.append(tiles[g] * scale)
    return jnp.concatenate(out, axis=0)[:, NB:]


def factor_kernel(scale, *refs):
    parts, (out_ref, second_ref, a_ref, m_ref) = refs[:-4], refs[-4:]
    n = out_ref.shape[0]
    total = parts[0][...].astype(F32)
    for part in parts[1:]:
        total += part[...].astype(F32)
    rows = total.shape[0] // 3
    a_ref[...] = unpacked((total[:rows] + total[rows : 2 * rows]) * scale)
    upper = unpacked(total[2 * rows :])
    index = [lax.broadcasted_iota(jnp.int32, (n, n), d) for d in (0, 1)]
    second_ref[...] = jnp.where(index[0] <= index[1], upper, upper.T)
    m_ref[...] = jnp.zeros((n, n), F32)
    out_ref[...] = jnp.zeros((n, n), F32)
    for lo in range(0, n, NB):
        hi = lo + NB
        inverse = factor_inverse(a_ref[lo:hi, lo:hi])
        out_ref[lo:hi, lo:hi] = inverse
        if lo:
            out_ref[lo:hi, :lo] = jnp.dot(inverse, m_ref[lo:hi, :lo], precision=HI, preferred_element_type=F32)
        if hi < n:
            upper = jnp.dot(inverse, a_ref[lo:hi, hi:], precision=HI, preferred_element_type=F32)
            a_ref[hi:, hi:] -= dot_tn(upper, upper, HI)
            m_ref[hi:, :hi] -= dot_tn(upper, out_ref[lo:hi, :hi], HI)


def final_kernel(scale, inv_ref, rows_ref, second_ref, sample_ref, image_ref, basis_ref, mapped_ref, ritz_ref):
    low = inv_ref[...].astype(BF16)
    basis_ref[...] = dot_nt(sample_ref[...], low).astype(BF16)
    mapped_ref[...] = dot_nt(image_ref[...], low).astype(BF16)
    left = jnp.dot(rows_ref[...], second_ref[...], precision=HI, preferred_element_type=F32)
    ritz_ref[...] = dot_nt(left, inv_ref[...], HI) * scale


def shifted(value, axis, by, wrap=True):
    count = lax.axis_size(axis)
    pairs = [(i, (i + by) % count) for i in range(count) if wrap or 0 <= i + by < count]
    return lax.ppermute(value, axis, pairs)


def added(*values):
    return sum(v.astype(F32) for v in values).astype(BF16)


def swapped(value):
    return lax.ppermute(value, "par", [(i, i ^ 1) for i in range(lax.axis_size("par"))])


def summed_over_par(keep, give):
    rows, width = keep.shape
    chips = lax.axis_size("par") // 2
    groups = [[2 * i + core for i in range(chips)] for core in range(2)]
    part = call(pair_kernel, "pair", shape(rows, width), [VMEM] * 2, [keep, swapped(give)], mib=4)
    exchange = lambda x: lax.all_to_all(x, "par", 0, 0, axis_index_groups=groups, tiled=True)
    parts = exchange(part.reshape(chips, rows // chips, width))
    own = call(total_kernel, "total", shape(*parts.shape), [VMEM], [parts], mib=4)
    mine = exchange(own).reshape(rows, width)
    return mine, swapped(mine)


def body(jacobian, probes, coeffs, offsets):
    ranks = lax.axis_size("obs")
    nobs, npar = jacobian.shape[0], jacobian.shape[1]
    width = probes.shape[1]
    count = coeffs.shape[0]
    me = jnp.stack([lax.axis_index("obs"), lax.axis_index("par") % 2])
    offsets = offsets.T
    flops = 2 * nobs * npar * width

    low, high = call(
        functools.partial(edges_kernel, count),
        "edges",
        [shape(nobs, EDGE)] * 2,
        [SMEM] + [VMEM] * 4,
        [offsets, jacobian[:, :EDGE], jacobian[:, npar - EDGE :], coeffs[:REACH], coeffs[count - REACH :]],
        [pltpu.VMEM((2 * REACH, nobs, BLK), F32)],
        mib=8,
        flops=flops // 4,
    )
    from_left = shifted(high, "par", 1, False)
    from_right = shifted(low, "par", -1, False)
    own = call(
        own_kernel,
        "own",
        shape(nobs, npar),
        [SMEM, VMEM, VMEM],
        [offsets, jacobian, coeffs],
        [pltpu.VMEM((count + 2 * REACH, nobs, BLK), F32)],
        flops=4 * flops,
    )
    half = shape(nobs // 2, width)
    full, keep, give = call(
        forward_kernel,
        "forward",
        [shape(nobs, npar), half, half],
        [SMEM] + [VMEM] * 4,
        [me, own, from_left, from_right, probes],
        flops=flops,
    )
    forward = summed_over_par(keep, give)

    pieces = call(
        functools.partial(sample_kernel, ranks),
        "sample",
        [shape(npar // ranks // 2, width)] * (2 * ranks),
        [SMEM] + [VMEM] * 3,
        [me, full, *forward],
        [pltpu.VMEM((nobs, width), BF16)],
        flops=flops,
    )
    here0, here1, right0, right1, far0, far1, left0, left1 = pieces
    via_left = shifted(far0, "obs", 1)
    via_right = shifted(far1, "obs", -1)
    a1 = shifted(right1, "obs", 1)
    b0 = shifted(left0, "obs", -1)
    a0 = shifted(added(right0, via_left), "obs", 1)
    b1 = shifted(added(left1, via_right), "obs", -1)
    sum0 = added(here0, a0, b0)
    sum1 = added(here1, a1, b1)

    l0 = shifted(sum0, "obs", 1)
    r1 = shifted(sum1, "obs", -1)
    l1 = shifted(sum1, "obs", 1)
    r0 = shifted(sum0, "obs", -1)
    f0 = shifted(l0, "obs", 1)
    f1 = shifted(r1, "obs", -1)

    edge = shape(EDGE, width)
    sample, tail_low, tail_high, keep, give = call(
        functools.partial(project_kernel, ranks),
        "project",
        [shape(npar, width), edge, edge, half, half],
        [SMEM] + [VMEM] * (1 + 2 * ranks),
        [me, full, sum0, sum1, r0, r1, f0, f1, l0, l1],
        [pltpu.VMEM((nobs, width), F32)],
        flops=flops,
    )
    below = shifted(tail_high, "par", 1, False)
    above = shifted(tail_low, "par", -1, False)
    projected = summed_over_par(keep, give)
    moments = call(
        moments_kernel,
        "moments",
        shape(15 * NB, 2 * NB),
        [SMEM] + [VMEM] * 4,
        [me, *forward, *projected],
        [pltpu.VMEM((nobs, width), BF16)] * 2,
        mib=8,
        flops=flops // 8,
    )
    parts = [moments] + [shifted(moments, "obs", by) for by in (1, -1, 2)]
    image = call(
        prior_kernel,
        "prior",
        shape(npar, width),
        [SMEM] + [VMEM] * 4,
        [offsets, coeffs, sample, below, above],
        [pltpu.VMEM((npar + 2 * EDGE, width), BF16)],
        mib=8,
        flops=flops,
    )
    total_par = npar * lax.axis_size("par")
    square = shape(width, width, dtype=F32)
    inverse, second = call(
        functools.partial(factor_kernel, 1.0 / total_par),
        "factor",
        [square, square],
        [VMEM] * len(parts),
        parts,
        [pltpu.VMEM((width, width), F32)] * 2,
        mib=8,
        flops=16 * flops,
    )
    steps = 4
    whole = pl.BlockSpec((width, width), lambda i: (0, 0))
    by_rows = pl.BlockSpec((npar // steps, width), lambda i: (i, 0))
    few = pl.BlockSpec((width // steps, width), lambda i: (i, 0))
    return pl.pallas_call(
        functools.partial(final_kernel, 1.0 / (nobs * ranks)),
        name="final",
        grid=(steps,),
        out_shape=[shape(npar, width), shape(npar, width), square],
        in_specs=[whole, few, whole, by_rows, by_rows],
        out_specs=[by_rows, by_rows, few],
        compiler_params=pltpu.CompilerParams(vmem_limit_bytes=12 * 2**20),
    )(inverse, inverse, second, sample, image)


def solution(mesh):
    return jax.shard_map(
        body,
        mesh=mesh,
        in_specs=(P("obs", "par"), P("par", None), P("par", None, None, None), P("par", None)),
        out_specs=(P("par", None), P("par", None), P()),
        check_vma=False,
    )
```

```python
import functools

import jax
import jax.numpy as jnp
from jax import lax
from jax.experimental import pallas as pl
from jax.experimental.pallas import tpu as pltpu
from jax.sharding import PartitionSpec as P


BLK = 128
REACH = 4
EDGE = REACH * BLK
NB = 64
F32 = jnp.float32
BF16 = jnp.bfloat16
HI = lax.Precision.HIGHEST
VMEM = pl.BlockSpec(memory_space=pltpu.VMEM)
SMEM = pl.BlockSpec(memory_space=pltpu.SMEM)


def core_index():
    return lax.rem(lax.axis_index("par"), 2)


def call(kernel, outs, specs, args, scratch=(), mib=24, flops=0):
    return pl.pallas_call(
        kernel,
        out_shape=outs,
        in_specs=specs,
        out_specs=jax.tree.map(lambda _: VMEM, outs),
        scratch_shapes=scratch,
        compiler_params=pltpu.CompilerParams(vmem_limit_bytes=mib * 2**20),
        cost_estimate=pl.CostEstimate(flops=flops, bytes_accessed=0, transcendentals=0),
    )(*args)


def dot(a, b):
    return jnp.dot(a, b, preferred_element_type=F32)


def dot_tn(a, b, precision=None):
    return lax.dot_general(a, b, (((0,), (0,)), ((), ())), precision=precision, preferred_element_type=F32)


def dot_nt(a, b, precision=None):
    return lax.dot_general(a, b, (((1,), (1,)), ((), ())), precision=precision, preferred_element_type=F32)


def shape(*dims, dtype=BF16):
    return jax.ShapeDtypeStruct(dims, dtype)


def edges_kernel(off_ref, jac_ref, coef_ref, partner_ref, neighbor_ref, acc):
    count = coef_ref.shape[0]
    acc[...] = jnp.zeros_like(acc)
    for side in range(2):
        for i in range(REACH):
            block = i + side * (count - REACH)
            columns = jac_ref[:, block * BLK : (block + 1) * BLK]
            for j in range(2):
                target = block + off_ref[j, block]
                place = target + REACH if side == 0 else target - count + REACH
                outside = target < 0 if side == 0 else target >= count

                @pl.when(outside)
                def _():
                    acc[place] += dot(columns, coef_ref[block, j + 1])

    core = core_index()
    for i in range(REACH):
        partner_ref[:, i * BLK : (i + 1) * BLK] = acc[(1 - core) * REACH + i].astype(BF16)
        neighbor_ref[:, i * BLK : (i + 1) * BLK] = acc[core * REACH + i].astype(BF16)


def own_kernel(off_ref, jac_ref, coef_ref, out_ref, acc):
    count = coef_ref.shape[0]
    for i in range(REACH):
        acc[i] = jnp.zeros_like(acc[i])
        acc[count + REACH + i] = jnp.zeros_like(acc[i])

    def diagonal(block, carry):
        columns = jac_ref[:, pl.ds(pl.multiple_of(block * BLK, BLK), BLK)]
        acc[block + REACH] = dot(columns, coef_ref[block, 0])
        return carry

    lax.fori_loop(0, count, diagonal, 0, unroll=4)

    def band(block, carry):
        columns = jac_ref[:, pl.ds(pl.multiple_of(block * BLK, BLK), BLK)]
        for j in range(2):
            acc[block + REACH + off_ref[j, block]] += dot(columns, coef_ref[block, j + 1])
        return carry

    lax.fori_loop(0, count, band, 0, unroll=4)
    for block in range(count):
        out_ref[:, block * BLK : (block + 1) * BLK] = acc[block + REACH].astype(BF16)


def halves(rows):
    core = core_index()
    return [pl.ds(pl.multiple_of(i * rows, rows), rows) for i in (core, 1 - core)]


def forward_kernel(own_ref, partner_ref, neighbor_ref, probe_ref, full_ref, keep_ref, give_ref, acc):
    width = own_ref.shape[1]
    core = core_index()
    full_ref[...] = own_ref[...]
    for come, side in ((partner_ref, 1 - core), (neighbor_ref, core)):
        here = pl.ds(pl.multiple_of(side * (width - EDGE), EDGE), EDGE)
        full_ref[:, here] = (own_ref[:, here].astype(F32) + come[...].astype(F32)).astype(BF16)
    acc[...] = dot(full_ref[...], probe_ref[...])
    mine, other = halves(keep_ref.shape[0])
    keep_ref[...] = acc[mine, :].astype(BF16)
    give_ref[...] = acc[other, :].astype(BF16)


def pair_kernel(keep_ref, come_ref, out_ref):
    out_ref[...] = (keep_ref[...].astype(F32) + come_ref[...].astype(F32)).astype(BF16)


def total_kernel(parts_ref, out_ref):
    total = parts_ref[0].astype(F32)
    for i in range(1, parts_ref.shape[0]):
        total += parts_ref[i].astype(F32)
    total = total.astype(BF16)
    for i in range(out_ref.shape[0]):
        out_ref[i] = total


def split(value):
    high = value.astype(BF16)
    return high, (value - high.astype(F32)).astype(BF16)


def joined(both):
    return both[:, :BLK].astype(F32) + both[:, BLK:].astype(F32)


def pair_gram_kernel(keep_ref, come_ref, out_ref):
    half = keep_ref.shape[0] // 2
    for i in range(out_ref.shape[0]):
        rows = slice(8 * i, 8 * i + 8)
        out_ref[i, :8] = (keep_ref[rows].astype(F32) + come_ref[rows].astype(F32)).astype(BF16)
        rows = slice(half + 8 * i, half + 8 * i + 8)
        out_ref[i, 8:, :BLK], out_ref[i, 8:, BLK:] = split(joined(keep_ref[rows]) + joined(come_ref[rows]))


def total_gram_kernel(parts_ref, out_ref):
    total = parts_ref[0].astype(F32)
    for i in range(1, parts_ref.shape[0]):
        total += parts_ref[i].astype(F32)
    rows = total[:8].astype(BF16)
    high, low = split(total[8:, :BLK] + total[8:, BLK:])
    for i in range(out_ref.shape[0]):
        out_ref[i, :8] = rows
        out_ref[i, 8:, :BLK] = high
        out_ref[i, 8:, BLK:] = low


def in_order(mine_ref, other_ref, out):
    for part, rows in zip((mine_ref, other_ref), halves(mine_ref.shape[0])):
        out[rows, :] = part[...]


def sample_kernel(ranks, full_ref, mine_ref, other_ref, *refs):
    outs, fwd = refs[:-1], refs[-1]
    rows = full_ref.shape[1] // ranks // 2
    in_order(mine_ref, other_ref, fwd)
    for rel in range(ranks):
        owner = lax.rem(lax.axis_index("obs") + rel, ranks)
        for half in range(2):
            start = pl.multiple_of(owner * (2 * rows) + half * rows, rows)
            outs[2 * rel + half][...] = dot_tn(full_ref[:, pl.ds(start, rows)], fwd[...]).astype(BF16)


def project_kernel(ranks, full_ref, *refs):
    pieces = refs[: 2 * ranks]
    sample_ref, neighbor_ref, keep_ref, give_ref, acc, gram = refs[2 * ranks :]
    rows = pieces[0].shape[0]
    total = jnp.zeros(acc.shape, F32)
    square = jnp.zeros(gram.shape, F32)
    for rel in range(ranks):
        owner = lax.rem(lax.axis_index("obs") + rel, ranks)
        for half in range(2):
            piece = pieces[2 * rel + half][...]
            start = pl.multiple_of(owner * (2 * rows) + half * rows, rows)
            sample_ref[pl.ds(start, rows), :] = piece
            total += dot(full_ref[:, pl.ds(start, rows)], piece)
            square += dot_tn(piece, piece)
    acc[...] = total
    gram[...] = square
    rows = acc.shape[0] // 2
    for out_ref, mine in zip((keep_ref, give_ref), halves(rows)):
        out_ref[:rows] = acc[mine, :].astype(BF16)
    for out_ref, mine in zip((keep_ref, give_ref), halves(BLK)):
        out_ref[rows : 2 * rows, :BLK], out_ref[rows : 2 * rows, BLK:] = split(gram[:, mine])
    core = core_index()
    last = sample_ref.shape[0] - EDGE
    neighbor_ref[...] = sample_ref[pl.ds(pl.multiple_of(core * last, EDGE), EDGE), :]
    give_ref[2 * rows :] = sample_ref[pl.ds(pl.multiple_of((1 - core) * last, EDGE), EDGE), :]


def prior_kernel(off_ref, coef_ref, sample_ref, come_ref, neighbor_ref, out_ref, ext):
    count, rows = coef_ref.shape[0], sample_ref.shape[0]
    core = core_index()
    far = EDGE + rows
    ext[EDGE : EDGE + rows] = sample_ref[...]
    ext[pl.ds(pl.multiple_of((1 - core) * far, EDGE), EDGE)] = come_ref[come_ref.shape[0] - EDGE :]
    ext[pl.ds(pl.multiple_of(core * far, EDGE), EDGE)] = neighbor_ref[...]

    def apply(block, carry):
        starts = [(block + REACH) * BLK] + [(block + REACH + off_ref[j, block]) * BLK for j in range(2)]
        result = sum(dot(coef_ref[block, j], ext[pl.ds(pl.multiple_of(starts[j], BLK), BLK), :]) for j in range(3))
        out_ref[pl.ds(pl.multiple_of(block * BLK, BLK), BLK), :] = result.astype(BF16)
        return carry

    lax.fori_loop(0, count, apply, 0, unroll=4)


def packed(full):
    return jnp.concatenate(
        [
            full[:NB, : 2 * NB],
            full[:NB, 2 * NB :],
            full[NB : 2 * NB, NB : 3 * NB],
            full[2 * NB : 3 * NB, 2 * NB :],
            jnp.concatenate([full[NB : 2 * NB, 3 * NB :], full[3 * NB :, 3 * NB :]], axis=1),
        ],
        axis=0,
    )


def unpacked(pack):
    r = [pack[i * NB : (i + 1) * NB] for i in range(5)]
    zero = jnp.zeros((NB, NB), F32)
    lane = lax.broadcasted_iota(jnp.int32, (NB, 2 * NB), 1)
    head = lambda block: jnp.where(lane < NB, 0.5, 1.0) * block
    join = lambda *p: jnp.concatenate(p, axis=1)
    return jnp.concatenate(
        [
            join(head(r[0]), r[1]),
            join(zero, head(r[2]), r[4][:, :NB]),
            join(zero, zero, head(r[3])),
            join(zero, zero, zero, 0.5 * r[4][:, NB:]),
        ],
        axis=0,
    )


def moments_kernel(mine_ref, other_ref, gram_ref, second_ref, proj):
    count = mine_ref.shape[0]
    for part, core in ((mine_ref, core_index()), (other_ref, 1 - core_index())):
        columns = pl.ds(pl.multiple_of(core * BLK, BLK), BLK)
        for i in range(count):
            proj[pl.ds(pl.multiple_of(core * (8 * count) + 8 * i, 8), 8), :] = part[i, :8].astype(F32)
            gram_ref[8 * i : 8 * i + 8, columns] = joined(part[i, 8:])
    rounded = proj[...].astype(BF16)
    second_ref[...] = packed(dot_tn(rounded, rounded)).astype(BF16)


def row_of(tile, k):
    return jnp.broadcast_to(tile[k : k + 1, :], tile.shape)


def lane_of(tile, k):
    return jnp.broadcast_to(tile[:, k : k + 1], (8, 2 * NB))


def factor_inverse(block):
    index = [lax.broadcasted_iota(jnp.int32, (NB, NB), d) for d in (0, 1)]
    wide = jnp.concatenate([block, (index[0] == index[1]).astype(F32)], axis=1)
    groups = NB // 8
    tiles = [wide[8 * t : 8 * t + 8] for t in range(groups)]
    row = lax.broadcasted_iota(jnp.int32, (8, 2 * NB), 0)
    out = []
    for g in range(groups):
        cols = {t: [lane_of(tiles[t], 8 * g + k) for k in range(8)] for t in range(g, groups)}
        done = tiles[g]
        for k in range(0, 8, 2):
            here = cols[g]
            p, q, r = row_of(here[k], k), row_of(here[k + 1], k), row_of(here[k + 1], k + 1)
            root = lax.rsqrt(p * r - q * q)
            inverse = root * root
            p_root = lax.rsqrt(p)
            row0, row1 = row_of(tiles[g], k), row_of(tiles[g], k + 1)
            second = (p * p_root * root) * (row1 - (q * p_root * p_root) * row0)
            done = jnp.where(row == k, p_root * row0, jnp.where(row == k + 1, second, done))
            head0 = [row_of(here[j], k) for j in range(k + 2, 8)]
            head1 = [row_of(here[j], k + 1) for j in range(k + 2, 8)]
            for t in range(g, groups):
                c0, c1 = cols[t][k], cols[t][k + 1]
                w0 = r * c0 - q * c1
                w1 = p * c1 - q * c0
                for j in range(k + 2, 8):
                    cols[t][j] = cols[t][j] - inverse * (w0 * head0[j - k - 2] + w1 * head1[j - k - 2])
                change = inverse * (w0 * row0 + w1 * row1)
                if t == g:
                    change = jnp.where(row > k + 1, change, 0.0)
                tiles[t] = tiles[t] - change
        out.append(done)
    return jnp.concatenate(out, axis=0)[:, NB:]


def exact(a, b, nt=False):
    return dot_nt(a, b, HI) if nt else jnp.dot(a, b, precision=HI, preferred_element_type=F32)


def factor_kernel(scale, gram_ref, out_ref, a_ref, m_ref, inv_ref):
    n = out_ref.shape[0]
    gram = gram_ref[...] * scale
    index = [lax.broadcasted_iota(jnp.int32, (n, n), d) for d in (0, 1)]
    diagonal = jnp.where(index[0] == index[1], gram, 0.0)
    across = lax.rsqrt(jnp.sum(diagonal, axis=0, keepdims=True))
    a_ref[...] = gram * across * lax.rsqrt(jnp.sum(diagonal, axis=1, keepdims=True))
    m_ref[...] = jnp.zeros((n, n), F32)
    inv_ref[...] = jnp.zeros((n, n), F32)
    for lo in range(0, n, NB):
        hi, nx = lo + NB, lo + 2 * NB
        inverse = factor_inverse(a_ref[lo:hi, lo:hi])
        inv_ref[lo:hi, lo:hi] = inverse
        if hi < n:
            upper = exact(inverse, a_ref[lo:hi, hi:])
            lower = exact(a_ref[hi:, lo:hi], inverse, nt=True)
            a_ref[hi:nx, hi:nx] -= exact(lower[:NB], upper[:, :NB])
            if nx < n:
                a_ref[hi:nx, nx:] -= exact(lower[:NB], upper[:, NB:])
                a_ref[nx:, hi:] -= exact(lower[NB:], upper)
        if lo:
            inv_ref[lo:hi, :lo] = exact(inverse, m_ref[lo:hi, :lo])
        if hi < n:
            m_ref[hi:, :hi] -= exact(lower, inv_ref[lo:hi, :hi])
    out_ref[...] = (inv_ref[...] * across).astype(BF16)


def final_kernel(scale, inv_ref, rows_ref, sample_ref, image_ref, *refs):
    seconds, (basis_ref, mapped_ref, ritz_ref) = refs[:-3], refs[-3:]
    inverse = inv_ref[...]
    basis_ref[...] = dot_nt(sample_ref[...], inverse).astype(BF16)
    mapped_ref[...] = dot_nt(image_ref[...], inverse).astype(BF16)
    total = seconds[0][...].astype(F32)
    for part in seconds[1:]:
        total += part[...].astype(F32)
    upper = unpacked(total).astype(BF16)
    left = dot(rows_ref[...], upper) + dot_nt(rows_ref[...], upper)
    ritz_ref[...] = dot_nt(left.astype(BF16), inverse) * scale


def shifted(value, axis, by):
    count = lax.axis_size(axis)
    return lax.ppermute(value, axis, [(i, (i + by) % count) for i in range(count)])


def to_neighbor(value):
    count = lax.axis_size("par")
    pairs = [pair for i in range(1, count - 1, 2) for pair in ((i, i + 1), (i + 1, i))]
    return lax.ppermute(value, "par", pairs)


def added(*values):
    return sum(v.astype(F32) for v in values).astype(BF16)


def swapped(value):
    return lax.ppermute(value, "par", [(i, i ^ 1) for i in range(lax.axis_size("par"))])


def exchanged(parts):
    groups = [[2 * i + core for i in range(parts.shape[0])] for core in range(2)]
    return lax.all_to_all(parts, "par", 0, 0, axis_index_groups=groups, tiled=True)


def body(jacobian, probes, coeffs, offsets):
    ranks = lax.axis_size("obs")
    chips = lax.axis_size("par") // 2
    nobs, npar = jacobian.shape[0], jacobian.shape[1]
    width = probes.shape[1]
    count = coeffs.shape[0]
    offsets = offsets.T
    flops = 2 * nobs * npar * width

    partner, neighbor = call(
        edges_kernel,
        [shape(nobs, EDGE)] * 2,
        [SMEM, VMEM, VMEM],
        [offsets, jacobian, coeffs],
        [pltpu.VMEM((2 * REACH, nobs, BLK), F32)],
        flops=flops // 4,
    )
    from_neighbor = to_neighbor(neighbor)
    from_partner = swapped(partner)
    own = call(
        own_kernel,
        shape(nobs, npar),
        [SMEM, VMEM, VMEM],
        [offsets, jacobian, coeffs],
        [pltpu.VMEM((count + 2 * REACH, nobs, BLK), F32)],
        flops=4 * flops,
    )
    half = shape(nobs // 2, width)
    full, keep, give = call(
        forward_kernel,
        [shape(nobs, npar), half, half],
        [VMEM] * 4,
        [own, from_partner, from_neighbor, probes],
        [pltpu.VMEM((nobs, width), F32)],
        mib=16,
        flops=flops,
    )
    part = call(pair_kernel, half, [VMEM] * 2, [keep, swapped(give)], mib=4)
    parts = exchanged(part.reshape(chips, nobs // 2 // chips, width))
    total = call(total_kernel, shape(*parts.shape), [VMEM], [parts], mib=4)
    mine = exchanged(total).reshape(half.shape)
    other = swapped(mine)

    pieces = call(
        functools.partial(sample_kernel, ranks),
        [shape(npar // ranks // 2, width)] * (2 * ranks),
        [VMEM] * 3,
        [full, mine, other],
        [pltpu.VMEM((nobs, width), BF16)],
        mib=16,
        flops=flops,
    )
    here0, here1, right0, right1, far0, far1, left0, left1 = pieces

    def ring(value, by):
        return shifted(value, "obs", by)

    via_left = ring(far0, 1)
    via_right = ring(far1, -1)
    a1 = ring(right1, 1)
    b0 = ring(left0, -1)
    a0 = ring(added(right0, via_left), 1)
    b1 = ring(added(left1, via_right), -1)
    sum0 = added(here0, a0, b0)
    sum1 = added(here1, a1, b1)

    l0 = ring(sum0, 1)
    r1 = ring(sum1, -1)
    l1 = ring(sum1, 1)
    r0 = ring(sum0, -1)
    f0 = ring(l0, 1)
    f1 = ring(r1, -1)

    sample, neighbor, keep, give = call(
        functools.partial(project_kernel, ranks),
        [shape(npar, width), shape(EDGE, width), shape(nobs, width), shape(nobs + EDGE, width)],
        [VMEM] * (1 + 2 * ranks),
        [full, sum0, sum1, r0, r1, f0, f1, l0, l1],
        [pltpu.VMEM((nobs, width), F32), pltpu.VMEM((width, width), F32)],
        mib=16,
        flops=flops,
    )
    come = swapped(give)
    from_neighbor = to_neighbor(neighbor)
    both = shape(chips, 16, width)
    part = call(pair_gram_kernel, both, [VMEM] * 2, [keep, come], mib=4)
    total = call(total_gram_kernel, both, [VMEM], [exchanged(part)], mib=4)
    mine = exchanged(total)
    other = swapped(mine)
    gram, second = call(
        moments_kernel,
        [shape(width, width, dtype=F32), shape(5 * NB, 2 * NB)],
        [VMEM] * 2,
        [mine, other],
        [pltpu.VMEM((nobs, width), F32)],
        mib=8,
        flops=flops // 8,
    )
    seconds = [second] + [shifted(second, "obs", by) for by in (1, -1, 2)]
    image = call(
        prior_kernel,
        shape(npar, width),
        [SMEM] + [VMEM] * 4,
        [offsets, coeffs, sample, come, from_neighbor],
        [pltpu.VMEM((npar + 2 * EDGE, width), BF16)],
        mib=8,
        flops=flops,
    )
    total_par = npar * lax.axis_size("par")
    inverse = call(
        functools.partial(factor_kernel, 1.0 / total_par),
        shape(width, width),
        [VMEM],
        [gram],
        [pltpu.VMEM((width, width), F32)] * 3,
        mib=8,
        flops=16 * flops,
    )
    steps = 4
    whole = lambda *dims: pl.BlockSpec(dims, lambda i: (0, 0))
    by_rows = pl.BlockSpec((npar // steps, width), lambda i: (i, 0))
    few = pl.BlockSpec((width // steps, width), lambda i: (i, 0))
    return pl.pallas_call(
        functools.partial(final_kernel, 1.0 / (nobs * ranks)),
        name="final",
        grid=(steps,),
        out_shape=[shape(npar, width), shape(npar, width), shape(width, width, dtype=F32)],
        in_specs=[whole(width, width), few, by_rows, by_rows] + [whole(*second.shape)] * len(seconds),
        out_specs=[by_rows, by_rows, few],
        compiler_params=pltpu.CompilerParams(vmem_limit_bytes=12 * 2**20),
    )(inverse, inverse, sample, image, *seconds)


def solution(mesh):
    return jax.shard_map(
        body,
        mesh=mesh,
        in_specs=(P("obs", "par"), P("par", None), P("par", None, None, None), P("par", None)),
        out_specs=(P("par", None), P("par", None), P()),
        check_vma=False,
    )
```

```python
import functools

import jax
import jax.numpy as jnp
from jax import lax
from jax.experimental import pallas as pl
from jax.experimental.pallas import tpu as pltpu
from jax.sharding import PartitionSpec as P


BLK = 128
REACH = 4
EDGE = REACH * BLK
NB = 64
F32 = jnp.float32
BF16 = jnp.bfloat16
HI = lax.Precision.HIGHEST
VMEM = pl.BlockSpec(memory_space=pltpu.VMEM)
SMEM = pl.BlockSpec(memory_space=pltpu.SMEM)


def core_index():
    return lax.rem(lax.axis_index("par"), 2)


def call(kernel, outs, specs, args, scratch=(), mib=24, flops=0):
    return pl.pallas_call(
        kernel,
        out_shape=outs,
        in_specs=specs,
        out_specs=jax.tree.map(lambda _: VMEM, outs),
        scratch_shapes=scratch,
        compiler_params=pltpu.CompilerParams(vmem_limit_bytes=mib * 2**20),
        cost_estimate=pl.CostEstimate(flops=flops, bytes_accessed=0, transcendentals=0),
    )(*args)


def dot(a, b):
    return jnp.dot(a, b, preferred_element_type=F32)


def dot_tn(a, b, precision=None):
    return lax.dot_general(a, b, (((0,), (0,)), ((), ())), precision=precision, preferred_element_type=F32)


def dot_nt(a, b, precision=None):
    return lax.dot_general(a, b, (((1,), (1,)), ((), ())), precision=precision, preferred_element_type=F32)


def shape(*dims, dtype=BF16):
    return jax.ShapeDtypeStruct(dims, dtype)


def edges_kernel(count, off_ref, jac_ref, coef_ref, partner_ref, neighbor_ref, acc):
    side = pl.program_id(0)
    acc[...] = jnp.zeros_like(acc)
    for i in range(REACH):
        block = i + side * (count - REACH)
        columns = jac_ref[:, i * BLK : (i + 1) * BLK]
        for j in range(2):
            target = block + off_ref[j, block]
            place = jnp.where(side == 0, target + REACH, target - count)

            @pl.when((place >= 0) & (place < REACH))
            def _():
                acc[place] += dot(columns, coef_ref[i, j + 1])

    for out_ref, wanted in ((partner_ref, 1 - core_index()), (neighbor_ref, core_index())):

        @pl.when(side == wanted)
        def _():
            for i in range(REACH):
                out_ref[:, i * BLK : (i + 1) * BLK] = acc[i].astype(BF16)


def own_kernel(off_ref, jac_ref, coef_ref, out_ref, acc):
    count = coef_ref.shape[0]
    for i in range(REACH):
        acc[i] = jnp.zeros_like(acc[i])
        acc[count + REACH + i] = jnp.zeros_like(acc[i])

    def diagonal(block, carry):
        columns = jac_ref[:, pl.ds(pl.multiple_of(block * BLK, BLK), BLK)]
        acc[block + REACH] = dot(columns, coef_ref[block, 0])
        return carry

    lax.fori_loop(0, count, diagonal, 0, unroll=8)

    def band(block, carry):
        columns = jac_ref[:, pl.ds(pl.multiple_of(block * BLK, BLK), BLK)]
        for j in range(2):
            acc[block + REACH + off_ref[j, block]] += dot(columns, coef_ref[block, j + 1])
        return carry

    lax.fori_loop(0, count, band, 0, unroll=8)
    for block in range(count):
        out_ref[:, block * BLK : (block + 1) * BLK] = acc[block + REACH].astype(BF16)


def halves(rows):
    core = core_index()
    return [pl.ds(pl.multiple_of(i * rows, rows), rows) for i in (core, 1 - core)]


def forward_kernel(own_ref, partner_ref, neighbor_ref, probe_ref, full_ref, keep_ref, give_ref, acc):
    width = own_ref.shape[1]
    core = core_index()
    full_ref[...] = own_ref[...]
    for come, side in ((partner_ref, 1 - core), (neighbor_ref, core)):
        here = pl.ds(pl.multiple_of(side * (width - EDGE), EDGE), EDGE)
        full_ref[:, here] = (own_ref[:, here].astype(F32) + come[...].astype(F32)).astype(BF16)
    acc[...] = dot(full_ref[...], probe_ref[...])
    mine, other = halves(keep_ref.shape[0])
    keep_ref[...] = acc[mine, :].astype(BF16)
    give_ref[...] = acc[other, :].astype(BF16)


def pair_kernel(keep_ref, come_ref, out_ref):
    out_ref[...] = (keep_ref[...].astype(F32) + come_ref[...].astype(F32)).astype(BF16)


def total_kernel(parts_ref, out_ref):
    total = parts_ref[0].astype(F32)
    for i in range(1, parts_ref.shape[0]):
        total += parts_ref[i].astype(F32)
    total = total.astype(BF16)
    for i in range(out_ref.shape[0]):
        out_ref[i] = total


def split(value):
    high = value.astype(BF16)
    return high, (value - high.astype(F32)).astype(BF16)


def joined(both):
    return both[:, :BLK].astype(F32) + both[:, BLK:].astype(F32)


def pair_gram_kernel(keep_ref, come_ref, out_ref):
    half = keep_ref.shape[0] // 2
    for i in range(out_ref.shape[0]):
        rows = slice(8 * i, 8 * i + 8)
        out_ref[i, :8] = (keep_ref[rows].astype(F32) + come_ref[rows].astype(F32)).astype(BF16)
        rows = slice(half + 8 * i, half + 8 * i + 8)
        out_ref[i, 8:, :BLK], out_ref[i, 8:, BLK:] = split(joined(keep_ref[rows]) + joined(come_ref[rows]))


def total_gram_kernel(parts_ref, out_ref):
    total = parts_ref[0].astype(F32)
    for i in range(1, parts_ref.shape[0]):
        total += parts_ref[i].astype(F32)
    rows = total[:8].astype(BF16)
    high, low = split(total[8:, :BLK] + total[8:, BLK:])
    for i in range(out_ref.shape[0]):
        out_ref[i, :8] = rows
        out_ref[i, 8:, :BLK] = high
        out_ref[i, 8:, BLK:] = low


def in_order(mine_ref, other_ref, out):
    for part, rows in zip((mine_ref, other_ref), halves(mine_ref.shape[0])):
        out[rows, :] = part[...]


def sample_kernel(ranks, full_ref, mine_ref, other_ref, *refs):
    outs, fwd = refs[:-1], refs[-1]
    rows = full_ref.shape[1] // ranks // 2
    in_order(mine_ref, other_ref, fwd)
    for rel in range(ranks):
        owner = lax.rem(lax.axis_index("obs") + rel, ranks)
        for half in range(2):
            start = pl.multiple_of(owner * (2 * rows) + half * rows, rows)
            outs[2 * rel + half][...] = dot_tn(full_ref[:, pl.ds(start, rows)], fwd[...]).astype(BF16)


def project_kernel(ranks, full_ref, *refs):
    pieces = refs[: 2 * ranks]
    sample_ref, neighbor_ref, keep_ref, give_ref, acc, gram = refs[2 * ranks :]
    rows = pieces[0].shape[0]
    total = jnp.zeros(acc.shape, F32)
    square = jnp.zeros(gram.shape, F32)
    for rel in range(ranks):
        owner = lax.rem(lax.axis_index("obs") + rel, ranks)
        for half in range(2):
            piece = pieces[2 * rel + half][...]
            start = pl.multiple_of(owner * (2 * rows) + half * rows, rows)
            sample_ref[pl.ds(start, rows), :] = piece
            total += dot(full_ref[:, pl.ds(start, rows)], piece)
            square += dot_tn(piece, piece)
    acc[...] = total
    gram[...] = square
    rows = acc.shape[0] // 2
    for out_ref, mine in zip((keep_ref, give_ref), halves(rows)):
        out_ref[:rows] = acc[mine, :].astype(BF16)
    for out_ref, mine in zip((keep_ref, give_ref), halves(BLK)):
        out_ref[rows : 2 * rows, :BLK], out_ref[rows : 2 * rows, BLK:] = split(gram[:, mine])
    core = core_index()
    last = sample_ref.shape[0] - EDGE
    neighbor_ref[...] = sample_ref[pl.ds(pl.multiple_of(core * last, EDGE), EDGE), :]
    give_ref[2 * rows :] = sample_ref[pl.ds(pl.multiple_of((1 - core) * last, EDGE), EDGE), :]


def prior_block(block, off_ref, coefs, ext, base):
    total = dot(coefs[0], ext[pl.ds(pl.multiple_of(base + block * BLK, BLK), BLK), :])
    for j in range(2):
        start = base + (block + off_ref[j, block]) * BLK
        total += dot(coefs[j + 1], ext[pl.ds(pl.multiple_of(start, BLK), BLK), :])
    return total.astype(BF16)


def outer_kernel(off_ref, coef_ref, sample_ref, come_ref, neighbor_ref, inv_ref, out_ref, ext):
    count, rows = coef_ref.shape[0], sample_ref.shape[0]
    core = core_index()
    ext[EDGE : 3 * EDGE] = sample_ref[: 2 * EDGE]
    ext[3 * EDGE : 5 * EDGE] = sample_ref[rows - 2 * EDGE :]
    ext[pl.ds(pl.multiple_of((1 - core) * (5 * EDGE), EDGE), EDGE)] = come_ref[come_ref.shape[0] - EDGE :]
    ext[pl.ds(pl.multiple_of(core * (5 * EDGE), EDGE), EDGE)] = neighbor_ref[...]
    for i in range(REACH):
        for side, base in ((0, EDGE), (1, 5 * EDGE - rows)):
            block = i + side * (count - REACH)
            coefs = [coef_ref[block, j] for j in range(3)]
            out_ref[side, i * BLK : (i + 1) * BLK] = prior_block(block, off_ref, coefs, ext, base)


def packed(full):
    return jnp.concatenate(
        [
            full[:NB, : 2 * NB],
            full[:NB, 2 * NB :],
            full[NB : 2 * NB, NB : 3 * NB],
            full[2 * NB : 3 * NB, 2 * NB :],
            jnp.concatenate([full[NB : 2 * NB, 3 * NB :], full[3 * NB :, 3 * NB :]], axis=1),
        ],
        axis=0,
    )


def unpacked(pack):
    r = [pack[i * NB : (i + 1) * NB] for i in range(5)]
    zero = jnp.zeros((NB, NB), F32)
    lane = lax.broadcasted_iota(jnp.int32, (NB, 2 * NB), 1)
    head = lambda block: jnp.where(lane < NB, 0.5, 1.0) * block
    join = lambda *p: jnp.concatenate(p, axis=1)
    return jnp.concatenate(
        [
            join(head(r[0]), r[1]),
            join(zero, head(r[2]), r[4][:, :NB]),
            join(zero, zero, head(r[3])),
            join(zero, zero, zero, 0.5 * r[4][:, NB:]),
        ],
        axis=0,
    )


def moments_kernel(mine_ref, other_ref, gram_ref, second_ref, proj):
    count = mine_ref.shape[0]
    for part, core in ((mine_ref, core_index()), (other_ref, 1 - core_index())):
        columns = pl.ds(pl.multiple_of(core * BLK, BLK), BLK)
        for i in range(count):
            proj[pl.ds(pl.multiple_of(core * (8 * count) + 8 * i, 8), 8), :] = part[i, :8].astype(F32)
            gram_ref[8 * i : 8 * i + 8, columns] = joined(part[i, 8:])
    rounded = proj[...].astype(BF16)
    second_ref[...] = packed(dot_tn(rounded, rounded)).astype(BF16)


def row_of(tile, k):
    return jnp.broadcast_to(tile[k : k + 1, :], tile.shape)


def lane_of(tile, k):
    return jnp.broadcast_to(tile[:, k : k + 1], (8, 2 * NB))


def factor_inverse(block):
    index = [lax.broadcasted_iota(jnp.int32, (NB, NB), d) for d in (0, 1)]
    wide = jnp.concatenate([block, (index[0] == index[1]).astype(F32)], axis=1)
    groups = NB // 8
    tiles = [wide[8 * t : 8 * t + 8] for t in range(groups)]
    row = lax.broadcasted_iota(jnp.int32, (8, 2 * NB), 0)
    out = []
    for g in range(groups):
        cols = {t: [lane_of(tiles[t], 8 * g + k) for k in range(8)] for t in range(g, groups)}
        done = tiles[g]
        for k in range(0, 8, 2):
            here = cols[g]
            p, q, r = row_of(here[k], k), row_of(here[k + 1], k), row_of(here[k + 1], k + 1)
            root = lax.rsqrt(p * r - q * q)
            inverse = root * root
            p_root = lax.rsqrt(p)
            row0, row1 = row_of(tiles[g], k), row_of(tiles[g], k + 1)
            second = (p * p_root * root) * (row1 - (q * p_root * p_root) * row0)
            done = jnp.where(row == k, p_root * row0, jnp.where(row == k + 1, second, done))
            head0 = [row_of(here[j], k) for j in range(k + 2, 8)]
            head1 = [row_of(here[j], k + 1) for j in range(k + 2, 8)]
            for t in range(g, groups):
                c0, c1 = cols[t][k], cols[t][k + 1]
                w0 = r * c0 - q * c1
                w1 = p * c1 - q * c0
                for j in range(k + 2, 8):
                    cols[t][j] = cols[t][j] - inverse * (w0 * head0[j - k - 2] + w1 * head1[j - k - 2])
                change = inverse * (w0 * row0 + w1 * row1)
                if t == g:
                    change = jnp.where(row > k + 1, change, 0.0)
                tiles[t] = tiles[t] - change
        out.append(done)
    return jnp.concatenate(out, axis=0)[:, NB:]


def exact(a, b, nt=False):
    return dot_nt(a, b, HI) if nt else jnp.dot(a, b, precision=HI, preferred_element_type=F32)


def factor_kernel(scale, gram_ref, off_ref, coef_ref, sample_ref, out_ref, image_ref, a_ref, m_ref, inv_ref):
    n = out_ref.shape[0]
    count = coef_ref.shape[0]
    inner = (count - 2 * REACH) * NB // n
    gram = gram_ref[...] * scale
    index = [lax.broadcasted_iota(jnp.int32, (n, n), d) for d in (0, 1)]
    diagonal = jnp.where(index[0] == index[1], gram, 0.0)
    across = lax.rsqrt(jnp.sum(diagonal, axis=0, keepdims=True))
    a_ref[...] = gram * across * lax.rsqrt(jnp.sum(diagonal, axis=1, keepdims=True))
    m_ref[...] = jnp.zeros((n, n), F32)
    inv_ref[...] = jnp.zeros((n, n), F32)
    for lo in range(0, n, NB):
        hi, nx = lo + NB, lo + 2 * NB
        inverse = factor_inverse(a_ref[lo:hi, lo:hi])
        inv_ref[lo:hi, lo:hi] = inverse
        first = REACH + lo // NB * inner
        for block in range(first, first + inner):
            coefs = [coef_ref[block, j] for j in range(3)]
            image_ref[block * BLK : (block + 1) * BLK] = prior_block(block, off_ref, coefs, sample_ref, 0)
        if hi < n:
            upper = exact(inverse, a_ref[lo:hi, hi:])
            lower = exact(a_ref[hi:, lo:hi], inverse, nt=True)
            a_ref[hi:nx, hi:nx] -= exact(lower[:NB], upper[:, :NB])
            if nx < n:
                a_ref[hi:nx, nx:] -= exact(lower[:NB], upper[:, NB:])
                a_ref[nx:, hi:] -= exact(lower[NB:], upper)
        if lo:
            inv_ref[lo:hi, :lo] = exact(inverse, m_ref[lo:hi, :lo])
        if hi < n:
            m_ref[hi:, :hi] -= exact(lower, inv_ref[lo:hi, :hi])
    out_ref[...] = (inv_ref[...] * across).astype(BF16)


def final_kernel(scale, inv_ref, rows_ref, sample_ref, image_ref, outer_ref, *refs):
    seconds, (basis_ref, mapped_ref, ritz_ref) = refs[:-3], refs[-3:]
    inverse = inv_ref[...]
    basis_ref[...] = dot_nt(sample_ref[...], inverse).astype(BF16)
    step, last = pl.program_id(0), pl.num_programs(0) - 1
    rows = image_ref.shape[0]
    top = jnp.where(step == 0, outer_ref[0], image_ref[:EDGE])
    bottom = jnp.where(step == last, outer_ref[1], image_ref[rows - EDGE :])
    mapped_ref[:EDGE] = dot_nt(top, inverse).astype(BF16)
    mapped_ref[rows - EDGE :] = dot_nt(bottom, inverse).astype(BF16)
    total = seconds[0][...].astype(F32)
    for part in seconds[1:]:
        total += part[...].astype(F32)
    upper = unpacked(total).astype(BF16)
    left = dot(rows_ref[...], upper) + dot_nt(rows_ref[...], upper)
    ritz_ref[...] = dot_nt(left.astype(BF16), inverse) * scale


def shifted(value, axis, by):
    count = lax.axis_size(axis)
    return lax.ppermute(value, axis, [(i, (i + by) % count) for i in range(count)])


def to_neighbor(value):
    count = lax.axis_size("par")
    pairs = [pair for i in range(1, count - 1, 2) for pair in ((i, i + 1), (i + 1, i))]
    return lax.ppermute(value, "par", pairs)


def added(*values):
    return sum(v.astype(F32) for v in values).astype(BF16)


def swapped(value):
    return lax.ppermute(value, "par", [(i, i ^ 1) for i in range(lax.axis_size("par"))])


def exchanged(parts):
    groups = [[2 * i + core for i in range(parts.shape[0])] for core in range(2)]
    return lax.all_to_all(parts, "par", 0, 0, axis_index_groups=groups, tiled=True)


def body(jacobian, probes, coeffs, offsets):
    ranks = lax.axis_size("obs")
    chips = lax.axis_size("par") // 2
    nobs, npar = jacobian.shape[0], jacobian.shape[1]
    width = probes.shape[1]
    count = coeffs.shape[0]
    offsets = offsets.T
    flops = 2 * nobs * npar * width

    whole = lambda *dims: pl.BlockSpec(dims, lambda i: (0,) * len(dims))
    last = npar // EDGE - 1
    partner, neighbor = pl.pallas_call(
        functools.partial(edges_kernel, count),
        name="edges",
        grid=(2,),
        out_shape=[shape(nobs, EDGE)] * 2,
        in_specs=[
            SMEM,
            pl.BlockSpec((nobs, EDGE), lambda i: (0, i * last)),
            pl.BlockSpec((REACH, *coeffs.shape[1:]), lambda i: (i * last, 0, 0, 0)),
        ],
        out_specs=[whole(nobs, EDGE)] * 2,
        scratch_shapes=[pltpu.VMEM((REACH, nobs, BLK), F32)],
        compiler_params=pltpu.CompilerParams(vmem_limit_bytes=50 * 2**20),
        cost_estimate=pl.CostEstimate(flops=flops // 4, bytes_accessed=0, transcendentals=0),
    )(offsets, jacobian, coeffs)
    from_neighbor = to_neighbor(neighbor)
    from_partner = swapped(partner)
    own = call(
        own_kernel,
        shape(nobs, npar),
        [SMEM, VMEM, VMEM],
        [offsets, jacobian, coeffs],
        [pltpu.VMEM((count + 2 * REACH, nobs, BLK), F32)],
        flops=4 * flops,
    )
    half = shape(nobs // 2, width)
    full, keep, give = call(
        forward_kernel,
        [shape(nobs, npar), half, half],
        [VMEM] * 4,
        [own, from_partner, from_neighbor, probes],
        [pltpu.VMEM((nobs, width), F32)],
        mib=16,
        flops=flops,
    )
    part = call(pair_kernel, half, [VMEM] * 2, [keep, swapped(give)], mib=4)
    parts = exchanged(part.reshape(chips, nobs // 2 // chips, width))
    total = call(total_kernel, shape(*parts.shape), [VMEM], [parts], mib=4)
    mine = exchanged(total).reshape(half.shape)
    other = swapped(mine)

    pieces = call(
        functools.partial(sample_kernel, ranks),
        [shape(npar // ranks // 2, width)] * (2 * ranks),
        [VMEM] * 3,
        [full, mine, other],
        [pltpu.VMEM((nobs, width), BF16)],
        mib=16,
        flops=flops,
    )
    here0, here1, right0, right1, far0, far1, left0, left1 = pieces

    def ring(value, by):
        return shifted(value, "obs", by)

    via_left = ring(far0, 1)
    via_right = ring(far1, -1)
    a1 = ring(right1, 1)
    b0 = ring(left0, -1)
    a0 = ring(added(right0, via_left), 1)
    b1 = ring(added(left1, via_right), -1)
    sum0 = added(here0, a0, b0)
    sum1 = added(here1, a1, b1)

    l0 = ring(sum0, 1)
    r1 = ring(sum1, -1)
    l1 = ring(sum1, 1)
    r0 = ring(sum0, -1)
    f0 = ring(l0, 1)
    f1 = ring(r1, -1)

    sample, neighbor, keep, give = call(
        functools.partial(project_kernel, ranks),
        [shape(npar, width), shape(EDGE, width), shape(nobs, width), shape(nobs + EDGE, width)],
        [VMEM] * (1 + 2 * ranks),
        [full, sum0, sum1, r0, r1, f0, f1, l0, l1],
        [pltpu.VMEM((nobs, width), F32), pltpu.VMEM((width, width), F32)],
        mib=16,
        flops=flops,
    )
    come = swapped(give)
    both = shape(chips, 16, width)
    part = call(pair_gram_kernel, both, [VMEM] * 2, [keep, come], mib=4)
    total = call(total_gram_kernel, both, [VMEM], [exchanged(part)], mib=4)
    mine = exchanged(total)
    other = swapped(mine)
    from_neighbor = to_neighbor(neighbor)
    gram, second = call(
        moments_kernel,
        [shape(width, width, dtype=F32), shape(5 * NB, 2 * NB)],
        [VMEM] * 2,
        [mine, other],
        [pltpu.VMEM((nobs, width), F32)],
        mib=8,
        flops=flops // 8,
    )
    seconds = [second] + [shifted(second, "obs", by) for by in (1, -1, 2)]
    total_par = npar * lax.axis_size("par")
    inverse, image = call(
        functools.partial(factor_kernel, 1.0 / total_par),
        [shape(width, width), shape(npar, width)],
        [VMEM, SMEM, VMEM, VMEM],
        [gram, offsets, coeffs, sample],
        [pltpu.VMEM((width, width), F32)] * 3,
        mib=16,
        flops=16 * flops,
    )
    outer = call(
        outer_kernel,
        shape(2, EDGE, width),
        [SMEM] + [VMEM] * 5,
        [offsets, coeffs, sample, come, from_neighbor, inverse],
        [pltpu.VMEM((6 * EDGE, width), BF16)],
        mib=16,
        flops=flops // 4,
    )
    steps = 4
    by_rows = pl.BlockSpec((npar // steps, width), lambda i: (i, 0))
    few = pl.BlockSpec((width // steps, width), lambda i: (i, 0))
    return pl.pallas_call(
        functools.partial(final_kernel, 1.0 / (nobs * ranks)),
        name="final",
        grid=(steps,),
        out_shape=[shape(npar, width), shape(npar, width), shape(width, width, dtype=F32)],
        in_specs=[whole(width, width), few, by_rows, by_rows, whole(2, EDGE, width)] + [whole(*second.shape)] * len(seconds),
        out_specs=[by_rows, by_rows, few],
        compiler_params=pltpu.CompilerParams(vmem_limit_bytes=12 * 2**20),
    )(inverse, inverse, sample, image, outer, *seconds)


def solution(mesh):
    return jax.shard_map(
        body,
        mesh=mesh,
        in_specs=(P("obs", "par"), P("par", None), P("par", None, None, None), P("par", None)),
        out_specs=(P("par", None), P("par", None), P()),
        check_vma=False,
    )
```

```python
import functools

import jax
import jax.numpy as jnp
from jax import lax
from jax.experimental import pallas as pl
from jax.experimental.pallas import tpu as pltpu
from jax.sharding import PartitionSpec as P


BLK = 128
REACH = 4
EDGE = REACH * BLK
NB = 64
F32 = jnp.float32
BF16 = jnp.bfloat16
HI = lax.Precision.HIGHEST
VMEM = pl.BlockSpec(memory_space=pltpu.VMEM)
SMEM = pl.BlockSpec(memory_space=pltpu.SMEM)


def core_index():
    return lax.rem(lax.axis_index("par"), 2)


def call(kernel, outs, specs, args, scratch=(), mib=24, flops=0):
    return pl.pallas_call(
        kernel,
        out_shape=outs,
        in_specs=specs,
        out_specs=jax.tree.map(lambda _: VMEM, outs),
        scratch_shapes=scratch,
        compiler_params=pltpu.CompilerParams(vmem_limit_bytes=mib * 2**20),
        cost_estimate=pl.CostEstimate(flops=flops, bytes_accessed=0, transcendentals=0),
    )(*args)


def dot(a, b):
    return jnp.dot(a, b, preferred_element_type=F32)


def dot_tn(a, b, precision=None):
    return lax.dot_general(a, b, (((0,), (0,)), ((), ())), precision=precision, preferred_element_type=F32)


def dot_nt(a, b, precision=None):
    return lax.dot_general(a, b, (((1,), (1,)), ((), ())), precision=precision, preferred_element_type=F32)


def shape(*dims, dtype=BF16):
    return jax.ShapeDtypeStruct(dims, dtype)


def edges_kernel(count, off_ref, jac_ref, coef_ref, partner_ref, neighbor_ref, acc):
    side = pl.program_id(0)
    acc[...] = jnp.zeros_like(acc)
    for i in range(REACH):
        block = i + side * (count - REACH)
        columns = jac_ref[:, i * BLK : (i + 1) * BLK]
        for j in range(2):
            target = block + off_ref[j, block]
            place = jnp.where(side == 0, target + REACH, target - count)

            @pl.when((place >= 0) & (place < REACH))
            def _():
                acc[place] += dot(columns, coef_ref[i, j + 1])

    for out_ref, wanted in ((partner_ref, 1 - core_index()), (neighbor_ref, core_index())):

        @pl.when(side == wanted)
        def _():
            for i in range(REACH):
                out_ref[:, i * BLK : (i + 1) * BLK] = acc[i].astype(BF16)


def own_kernel(off_ref, jac_ref, coef_ref, out_ref, acc):
    count = coef_ref.shape[0]
    for i in range(REACH):
        acc[i] = jnp.zeros_like(acc[i])
        acc[count + REACH + i] = jnp.zeros_like(acc[i])

    def diagonal(block, carry):
        columns = jac_ref[:, pl.ds(pl.multiple_of(block * BLK, BLK), BLK)]
        acc[block + REACH] = dot(columns, coef_ref[block, 0])
        return carry

    lax.fori_loop(0, count, diagonal, 0, unroll=8)

    def band(block, carry):
        columns = jac_ref[:, pl.ds(pl.multiple_of(block * BLK, BLK), BLK)]
        for j in range(2):
            acc[block + REACH + off_ref[j, block]] += dot(columns, coef_ref[block, j + 1])
        return carry

    lax.fori_loop(0, count, band, 0, unroll=8)
    for block in range(count):
        place = block % REACH
        out_ref[block // REACH, :, place * BLK : (place + 1) * BLK] = acc[block + REACH].astype(BF16)


def inner_kernel(own_ref, probe_ref, out_ref):
    chunks = own_ref.shape[0]
    out_ref[...] = sum(dot(own_ref[i], probe_ref[i * EDGE : (i + 1) * EDGE, :]) for i in range(1, chunks - 1))


def halves(rows):
    core = core_index()
    return [pl.ds(pl.multiple_of(i * rows, rows), rows) for i in (core, 1 - core)]


def forward_kernel(own_ref, partner_ref, neighbor_ref, probe_ref, inner_ref, full_ref, keep_ref, give_ref, acc):
    side = pl.program_id(0)
    come = jnp.where(side == 1 - core_index(), partner_ref[...], neighbor_ref[...])
    chunk = (own_ref[0].astype(F32) + come.astype(F32)).astype(BF16)
    full_ref[0] = chunk
    product = dot(chunk, probe_ref[...])

    @pl.when(side == 0)
    def _():
        acc[...] = inner_ref[...] + product

    @pl.when(side == 1)
    def _():
        acc[...] += product
        mine, other = halves(keep_ref.shape[0])
        keep_ref[...] = acc[mine, :].astype(BF16)
        give_ref[...] = acc[other, :].astype(BF16)


def pair_kernel(keep_ref, come_ref, out_ref):
    out_ref[...] = (keep_ref[...].astype(F32) + come_ref[...].astype(F32)).astype(BF16)


def total_kernel(parts_ref, out_ref):
    total = parts_ref[0].astype(F32)
    for i in range(1, parts_ref.shape[0]):
        total += parts_ref[i].astype(F32)
    total = total.astype(BF16)
    for i in range(out_ref.shape[0]):
        out_ref[i] = total


def split(value):
    high = value.astype(BF16)
    return high, (value - high.astype(F32)).astype(BF16)


def joined(both):
    return both[:, :BLK].astype(F32) + both[:, BLK:].astype(F32)


def pair_gram_kernel(keep_ref, come_ref, out_ref):
    half = keep_ref.shape[0] // 2
    for i in range(out_ref.shape[0]):
        rows = slice(8 * i, 8 * i + 8)
        out_ref[i, :8] = (keep_ref[rows].astype(F32) + come_ref[rows].astype(F32)).astype(BF16)
        rows = slice(half + 8 * i, half + 8 * i + 8)
        out_ref[i, 8:, :BLK], out_ref[i, 8:, BLK:] = split(joined(keep_ref[rows]) + joined(come_ref[rows]))


def total_gram_kernel(parts_ref, out_ref):
    total = parts_ref[0].astype(F32)
    for i in range(1, parts_ref.shape[0]):
        total += parts_ref[i].astype(F32)
    rows = total[:8].astype(BF16)
    high, low = split(total[8:, :BLK] + total[8:, BLK:])
    for i in range(out_ref.shape[0]):
        out_ref[i, :8] = rows
        out_ref[i, 8:, :BLK] = high
        out_ref[i, 8:, BLK:] = low


def in_order(mine_ref, other_ref, out):
    for part, rows in zip((mine_ref, other_ref), halves(mine_ref.shape[0])):
        out[rows, :] = part[...]


def sample_kernel(ranks, full_ref, mine_ref, other_ref, *refs):
    outs, fwd = refs[:-1], refs[-1]
    in_order(mine_ref, other_ref, fwd)
    for rel in range(ranks):
        owner = lax.rem(lax.axis_index("obs") + rel, ranks)
        for half in range(2):
            outs[2 * rel + half][...] = dot_tn(full_ref[2 * owner + half], fwd[...]).astype(BF16)


def project_kernel(ranks, full_ref, *refs):
    pieces = refs[: 2 * ranks]
    sample_ref, neighbor_ref, keep_ref, give_ref, acc, gram = refs[2 * ranks :]
    rows = pieces[0].shape[0]
    total = jnp.zeros(acc.shape, F32)
    square = jnp.zeros(gram.shape, F32)
    for rel in range(ranks):
        owner = lax.rem(lax.axis_index("obs") + rel, ranks)
        for half in range(2):
            piece = pieces[2 * rel + half][...]
            start = pl.multiple_of(owner * (2 * rows) + half * rows, rows)
            sample_ref[pl.ds(start, rows), :] = piece
            total += dot(full_ref[2 * owner + half], piece)
            square += dot_tn(piece, piece)
    acc[...] = total
    gram[...] = square
    rows = acc.shape[0] // 2
    for out_ref, mine in zip((keep_ref, give_ref), halves(rows)):
        out_ref[:rows] = acc[mine, :].astype(BF16)
    for out_ref, mine in zip((keep_ref, give_ref), halves(BLK)):
        out_ref[rows : 2 * rows, :BLK], out_ref[rows : 2 * rows, BLK:] = split(gram[:, mine])
    core = core_index()
    last = sample_ref.shape[0] - EDGE
    neighbor_ref[...] = sample_ref[pl.ds(pl.multiple_of(core * last, EDGE), EDGE), :]
    give_ref[2 * rows :] = sample_ref[pl.ds(pl.multiple_of((1 - core) * last, EDGE), EDGE), :]


def prior_block(block, off_ref, coefs, ext, base):
    total = dot(coefs[0], ext[pl.ds(pl.multiple_of(base + block * BLK, BLK), BLK), :])
    for j in range(2):
        start = base + (block + off_ref[j, block]) * BLK
        total += dot(coefs[j + 1], ext[pl.ds(pl.multiple_of(start, BLK), BLK), :])
    return total.astype(BF16)


def fill_ends(sample_ref, come_ref, neighbor_ref, ext):
    rows = sample_ref.shape[0]
    core = core_index()
    ext[EDGE : 3 * EDGE] = sample_ref[: 2 * EDGE]
    ext[3 * EDGE : 5 * EDGE] = sample_ref[rows - 2 * EDGE :]
    ext[pl.ds(pl.multiple_of((1 - core) * (5 * EDGE), EDGE), EDGE)] = come_ref[come_ref.shape[0] - EDGE :]
    ext[pl.ds(pl.multiple_of(core * (5 * EDGE), EDGE), EDGE)] = neighbor_ref[...]


def packed(full):
    return jnp.concatenate(
        [
            full[:NB, : 2 * NB],
            full[:NB, 2 * NB :],
            full[NB : 2 * NB, NB : 3 * NB],
            full[2 * NB : 3 * NB, 2 * NB :],
            jnp.concatenate([full[NB : 2 * NB, 3 * NB :], full[3 * NB :, 3 * NB :]], axis=1),
        ],
        axis=0,
    )


def unpacked(pack):
    r = [pack[i * NB : (i + 1) * NB] for i in range(5)]
    zero = jnp.zeros((NB, NB), F32)
    lane = lax.broadcasted_iota(jnp.int32, (NB, 2 * NB), 1)
    head = lambda block: jnp.where(lane < NB, 0.5, 1.0) * block
    join = lambda *p: jnp.concatenate(p, axis=1)
    return jnp.concatenate(
        [
            join(head(r[0]), r[1]),
            join(zero, head(r[2]), r[4][:, :NB]),
            join(zero, zero, head(r[3])),
            join(zero, zero, zero, 0.5 * r[4][:, NB:]),
        ],
        axis=0,
    )


def moments_kernel(mine_ref, other_ref, gram_ref, second_ref, proj):
    count = mine_ref.shape[0]
    for part, core in ((mine_ref, core_index()), (other_ref, 1 - core_index())):
        columns = pl.ds(pl.multiple_of(core * BLK, BLK), BLK)
        for i in range(count):
            proj[pl.ds(pl.multiple_of(core * (8 * count) + 8 * i, 8), 8), :] = part[i, :8].astype(F32)
            gram_ref[8 * i : 8 * i + 8, columns] = joined(part[i, 8:])
    rounded = proj[...].astype(BF16)
    second_ref[...] = packed(dot_tn(rounded, rounded)).astype(BF16)


def row_of(tile, k):
    return jnp.broadcast_to(tile[k : k + 1, :], tile.shape)


def lane_of(tile, k):
    return jnp.broadcast_to(tile[:, k : k + 1], (8, 2 * NB))


def factor_inverse(block):
    index = [lax.broadcasted_iota(jnp.int32, (NB, NB), d) for d in (0, 1)]
    wide = jnp.concatenate([block, (index[0] == index[1]).astype(F32)], axis=1)
    groups = NB // 8
    tiles = [wide[8 * t : 8 * t + 8] for t in range(groups)]
    row = lax.broadcasted_iota(jnp.int32, (8, 2 * NB), 0)
    out = []
    for g in range(groups):
        cols = {t: [lane_of(tiles[t], 8 * g + k) for k in range(8)] for t in range(g, groups)}
        done = tiles[g]
        for k in range(0, 8, 2):
            here = cols[g]
            p, q, r = row_of(here[k], k), row_of(here[k + 1], k), row_of(here[k + 1], k + 1)
            root = lax.rsqrt(p * r - q * q)
            inverse = root * root
            p_root = lax.rsqrt(p)
            row0, row1 = row_of(tiles[g], k), row_of(tiles[g], k + 1)
            second = (p * p_root * root) * (row1 - (q * p_root * p_root) * row0)
            done = jnp.where(row == k, p_root * row0, jnp.where(row == k + 1, second, done))
            head0 = [row_of(here[j], k) for j in range(k + 2, 8)]
            head1 = [row_of(here[j], k + 1) for j in range(k + 2, 8)]
            for t in range(g, groups):
                c0, c1 = cols[t][k], cols[t][k + 1]
                w0 = r * c0 - q * c1
                w1 = p * c1 - q * c0
                for j in range(k + 2, 8):
                    cols[t][j] = cols[t][j] - inverse * (w0 * head0[j - k - 2] + w1 * head1[j - k - 2])
                change = inverse * (w0 * row0 + w1 * row1)
                if t == g:
                    change = jnp.where(row > k + 1, change, 0.0)
                tiles[t] = tiles[t] - change
        out.append(done)
    return jnp.concatenate(out, axis=0)[:, NB:]


def exact(a, b, nt=False):
    return dot_nt(a, b, HI) if nt else jnp.dot(a, b, precision=HI, preferred_element_type=F32)


def factor_kernel(
    scale, gram_ref, off_ref, coef_ref, sample_ref, come_ref, neighbor_ref, out_ref, image_ref, a_ref, m_ref, inv_ref, ext
):
    n = out_ref.shape[0]
    count, rows = coef_ref.shape[0], sample_ref.shape[0]
    share = count * NB // n
    fill_ends(sample_ref, come_ref, neighbor_ref, ext)
    gram = gram_ref[...] * scale
    index = [lax.broadcasted_iota(jnp.int32, (n, n), d) for d in (0, 1)]
    diagonal = jnp.where(index[0] == index[1], gram, 0.0)
    across = lax.rsqrt(jnp.sum(diagonal, axis=0, keepdims=True))
    a_ref[...] = gram * across * lax.rsqrt(jnp.sum(diagonal, axis=1, keepdims=True))
    m_ref[...] = jnp.zeros((n, n), F32)
    inv_ref[...] = jnp.zeros((n, n), F32)
    for lo in range(0, n, NB):
        hi, nx = lo + NB, lo + 2 * NB
        inverse = factor_inverse(a_ref[lo:hi, lo:hi])
        inv_ref[lo:hi, lo:hi] = inverse
        first = lo // NB * share
        for block in range(first, first + share):
            coefs = [coef_ref[block, j] for j in range(3)]
            source, base = sample_ref, 0
            if block < REACH:
                source, base = ext, EDGE
            elif block >= count - REACH:
                source, base = ext, 5 * EDGE - rows
            image_ref[block * BLK : (block + 1) * BLK] = prior_block(block, off_ref, coefs, source, base)
        if hi < n:
            upper = exact(inverse, a_ref[lo:hi, hi:])
            lower = exact(a_ref[hi:, lo:hi], inverse, nt=True)
            a_ref[hi:nx, hi:nx] -= exact(lower[:NB], upper[:, :NB])
            if nx < n:
                a_ref[hi:nx, nx:] -= exact(lower[:NB], upper[:, NB:])
                a_ref[nx:, hi:] -= exact(lower[NB:], upper)
        if lo:
            inv_ref[lo:hi, :lo] = exact(inverse, m_ref[lo:hi, :lo])
        if hi < n:
            m_ref[hi:, :hi] -= exact(lower, inv_ref[lo:hi, :hi])
    out_ref[...] = (inv_ref[...] * across).astype(BF16)


def final_kernel(scale, inv_ref, rows_ref, sample_ref, image_ref, *refs):
    seconds, (basis_ref, mapped_ref, ritz_ref) = refs[:-3], refs[-3:]
    inverse = inv_ref[...]
    basis_ref[...] = dot_nt(sample_ref[...], inverse).astype(BF16)
    mapped_ref[...] = dot_nt(image_ref[...], inverse).astype(BF16)
    total = seconds[0][...].astype(F32)
    for part in seconds[1:]:
        total += part[...].astype(F32)
    upper = unpacked(total).astype(BF16)
    left = dot(rows_ref[...], upper) + dot_nt(rows_ref[...], upper)
    ritz_ref[...] = dot_nt(left.astype(BF16), inverse) * scale


def shifted(value, axis, by):
    count = lax.axis_size(axis)
    return lax.ppermute(value, axis, [(i, (i + by) % count) for i in range(count)])


def to_neighbor(value):
    count = lax.axis_size("par")
    pairs = [pair for i in range(1, count - 1, 2) for pair in ((i, i + 1), (i + 1, i))]
    return lax.ppermute(value, "par", pairs)


def added(*values):
    return sum(v.astype(F32) for v in values).astype(BF16)


def swapped(value):
    return lax.ppermute(value, "par", [(i, i ^ 1) for i in range(lax.axis_size("par"))])


def exchanged(parts):
    groups = [[2 * i + core for i in range(parts.shape[0])] for core in range(2)]
    return lax.all_to_all(parts, "par", 0, 0, axis_index_groups=groups, tiled=True)


def body(jacobian, probes, coeffs, offsets):
    ranks = lax.axis_size("obs")
    chips = lax.axis_size("par") // 2
    nobs, npar = jacobian.shape[0], jacobian.shape[1]
    width = probes.shape[1]
    count = coeffs.shape[0]
    offsets = offsets.T
    flops = 2 * nobs * npar * width

    whole = lambda *dims: pl.BlockSpec(dims, lambda i: (0,) * len(dims))
    chunks = npar // EDGE
    last = chunks - 1
    partner, neighbor = pl.pallas_call(
        functools.partial(edges_kernel, count),
        name="edges",
        grid=(2,),
        out_shape=[shape(nobs, EDGE)] * 2,
        in_specs=[
            SMEM,
            pl.BlockSpec((nobs, EDGE), lambda i: (0, i * last)),
            pl.BlockSpec((REACH, *coeffs.shape[1:]), lambda i: (i * last, 0, 0, 0)),
        ],
        out_specs=[whole(nobs, EDGE)] * 2,
        scratch_shapes=[pltpu.VMEM((REACH, nobs, BLK), F32)],
        compiler_params=pltpu.CompilerParams(vmem_limit_bytes=50 * 2**20),
        cost_estimate=pl.CostEstimate(flops=flops // 4, bytes_accessed=0, transcendentals=0),
    )(offsets, jacobian, coeffs)
    from_neighbor = to_neighbor(neighbor)
    from_partner = swapped(partner)
    own = call(
        own_kernel,
        shape(chunks, nobs, EDGE),
        [SMEM, VMEM, VMEM],
        [offsets, jacobian, coeffs],
        [pltpu.VMEM((count + 2 * REACH, nobs, BLK), F32)],
        flops=4 * flops,
    )
    half = shape(nobs // 2, width)
    inner = call(inner_kernel, shape(nobs, width, dtype=F32), [VMEM] * 2, [own, probes], flops=flops)
    edge_chunk = pl.BlockSpec((1, nobs, EDGE), lambda i: (i * last, 0, 0))
    full, keep, give = pl.pallas_call(
        forward_kernel,
        name="forward",
        grid=(2,),
        out_shape=[shape(chunks, nobs, EDGE), half, half],
        in_specs=[
            edge_chunk,
            whole(nobs, EDGE),
            whole(nobs, EDGE),
            pl.BlockSpec((EDGE, width), lambda i: (i * last, 0)),
            whole(nobs, width),
        ],
        out_specs=[edge_chunk, whole(*half.shape), whole(*half.shape)],
        scratch_shapes=[pltpu.VMEM((nobs, width), F32)],
        input_output_aliases={0: 0},
        compiler_params=pltpu.CompilerParams(vmem_limit_bytes=24 * 2**20),
    )(own, from_partner, from_neighbor, probes, inner)
    part = call(pair_kernel, half, [VMEM] * 2, [keep, swapped(give)], mib=4)
    parts = exchanged(part.reshape(chips, nobs // 2 // chips, width))
    total = call(total_kernel, shape(*parts.shape), [VMEM], [parts], mib=4)
    mine = exchanged(total).reshape(half.shape)
    other = swapped(mine)

    pieces = call(
        functools.partial(sample_kernel, ranks),
        [shape(npar // ranks // 2, width)] * (2 * ranks),
        [VMEM] * 3,
        [full, mine, other],
        [pltpu.VMEM((nobs, width), BF16)],
        mib=16,
        flops=flops,
    )
    here0, here1, right0, right1, far0, far1, left0, left1 = pieces

    def ring(value, by):
        return shifted(value, "obs", by)

    via_left = ring(far0, 1)
    via_right = ring(far1, -1)
    a1 = ring(right1, 1)
    b0 = ring(left0, -1)
    a0 = ring(added(right0, via_left), 1)
    b1 = ring(added(left1, via_right), -1)
    sum0 = added(here0, a0, b0)
    sum1 = added(here1, a1, b1)

    l0 = ring(sum0, 1)
    r1 = ring(sum1, -1)
    l1 = ring(sum1, 1)
    r0 = ring(sum0, -1)
    f0 = ring(l0, 1)
    f1 = ring(r1, -1)

    sample, neighbor, keep, give = call(
        functools.partial(project_kernel, ranks),
        [shape(npar, width), shape(EDGE, width), shape(nobs, width), shape(nobs + EDGE, width)],
        [VMEM] * (1 + 2 * ranks),
        [full, sum0, sum1, r0, r1, f0, f1, l0, l1],
        [pltpu.VMEM((nobs, width), F32), pltpu.VMEM((width, width), F32)],
        mib=16,
        flops=flops,
    )
    come = swapped(give)
    both = shape(chips, 16, width)
    part = call(pair_gram_kernel, both, [VMEM] * 2, [keep, come], mib=4)
    total = call(total_gram_kernel, both, [VMEM], [exchanged(part)], mib=4)
    mine = exchanged(total)
    other = swapped(mine)
    from_neighbor = to_neighbor(neighbor)
    gram, second = call(
        moments_kernel,
        [shape(width, width, dtype=F32), shape(5 * NB, 2 * NB)],
        [VMEM] * 2,
        [mine, other],
        [pltpu.VMEM((nobs, width), F32)],
        mib=8,
        flops=flops // 8,
    )
    seconds = [second] + [shifted(second, "obs", by) for by in (1, -1, 2)]
    total_par = npar * lax.axis_size("par")
    inverse, image = call(
        functools.partial(factor_kernel, 1.0 / total_par),
        [shape(width, width), shape(npar, width)],
        [VMEM, SMEM] + [VMEM] * 4,
        [gram, offsets, coeffs, sample, come, from_neighbor],
        [pltpu.VMEM((width, width), F32)] * 3 + [pltpu.VMEM((6 * EDGE, width), BF16)],
        mib=16,
        flops=16 * flops,
    )
    steps = 4
    by_rows = pl.BlockSpec((npar // steps, width), lambda i: (i, 0))
    few = pl.BlockSpec((width // steps, width), lambda i: (i, 0))
    return pl.pallas_call(
        functools.partial(final_kernel, 1.0 / (nobs * ranks)),
        name="final",
        grid=(steps,),
        out_shape=[shape(npar, width), shape(npar, width), shape(width, width, dtype=F32)],
        in_specs=[whole(width, width), few, by_rows, by_rows] + [whole(*second.shape)] * len(seconds),
        out_specs=[by_rows, by_rows, few],
        compiler_params=pltpu.CompilerParams(vmem_limit_bytes=12 * 2**20),
    )(inverse, inverse, sample, image, *seconds)


def solution(mesh):
    return jax.shard_map(
        body,
        mesh=mesh,
        in_specs=(P("obs", "par"), P("par", None), P("par", None, None, None), P("par", None)),
        out_specs=(P("par", None), P("par", None), P()),
        check_vma=False,
    )
```

```python
import functools

import jax
import jax.numpy as jnp
from jax import lax
from jax.experimental import pallas as pl
from jax.experimental.pallas import tpu as pltpu
from jax.sharding import PartitionSpec as P


BLK = 128
REACH = 4
EDGE = REACH * BLK
NB = 64
F32 = jnp.float32
BF16 = jnp.bfloat16
HI = lax.Precision.HIGHEST
VMEM = pl.BlockSpec(memory_space=pltpu.VMEM)
SMEM = pl.BlockSpec(memory_space=pltpu.SMEM)


def core_index():
    return lax.rem(lax.axis_index("par"), 2)


def call(kernel, outs, specs, args, scratch=(), mib=24, flops=0):
    return pl.pallas_call(
        kernel,
        out_shape=outs,
        in_specs=specs,
        out_specs=jax.tree.map(lambda _: VMEM, outs),
        scratch_shapes=scratch,
        compiler_params=pltpu.CompilerParams(vmem_limit_bytes=mib * 2**20),
        cost_estimate=pl.CostEstimate(flops=flops, bytes_accessed=0, transcendentals=0),
    )(*args)


def dot(a, b):
    return jnp.dot(a, b, preferred_element_type=F32)


def dot_tn(a, b, precision=None):
    return lax.dot_general(a, b, (((0,), (0,)), ((), ())), precision=precision, preferred_element_type=F32)


def dot_nt(a, b, precision=None):
    return lax.dot_general(a, b, (((1,), (1,)), ((), ())), precision=precision, preferred_element_type=F32)


def shape(*dims, dtype=BF16):
    return jax.ShapeDtypeStruct(dims, dtype)


def edges_kernel(count, off_ref, jac_ref, coef_ref, partner_ref, neighbor_ref, acc):
    side = pl.program_id(0)
    acc[...] = jnp.zeros_like(acc)
    for i in range(REACH):
        block = i + side * (count - REACH)
        columns = jac_ref[:, i * BLK : (i + 1) * BLK]
        for j in range(2):
            target = block + off_ref[j, block]
            place = jnp.where(side == 0, target + REACH, target - count)

            @pl.when((place >= 0) & (place < REACH))
            def _():
                acc[place] += dot(columns, coef_ref[i, j + 1])

    for out_ref, wanted in ((partner_ref, 1 - core_index()), (neighbor_ref, core_index())):

        @pl.when(side == wanted)
        def _():
            for i in range(REACH):
                out_ref[:, i * BLK : (i + 1) * BLK] = acc[i].astype(BF16)


def own_kernel(off_ref, jac_ref, coef_ref, out_ref, acc):
    count = coef_ref.shape[0]
    for i in range(REACH):
        acc[i] = jnp.zeros_like(acc[i])
        acc[count + REACH + i] = jnp.zeros_like(acc[i])

    def diagonal(block, carry):
        columns = jac_ref[:, pl.ds(pl.multiple_of(block * BLK, BLK), BLK)]
        acc[block + REACH] = dot(columns, coef_ref[block, 0])
        return carry

    lax.fori_loop(0, count, diagonal, 0, unroll=8)

    def band(block, carry):
        columns = jac_ref[:, pl.ds(pl.multiple_of(block * BLK, BLK), BLK)]
        for j in range(2):
            acc[block + REACH + off_ref[j, block]] += dot(columns, coef_ref[block, j + 1])
        return carry

    lax.fori_loop(0, count, band, 0, unroll=8)
    for block in range(count):
        place = block % REACH
        out_ref[block // REACH, :, place * BLK : (place + 1) * BLK] = acc[block + REACH].astype(BF16)


def inner_kernel(own_ref, probe_ref, out_ref):
    chunks = own_ref.shape[0]
    out_ref[...] = sum(dot(own_ref[i], probe_ref[i * EDGE : (i + 1) * EDGE, :]) for i in range(1, chunks - 1))


def halves(rows):
    core = core_index()
    return [pl.ds(pl.multiple_of(i * rows, rows), rows) for i in (core, 1 - core)]


def forward_kernel(own_ref, partner_ref, neighbor_ref, probe_ref, inner_ref, full_ref, keep_ref, give_ref, acc):
    side = pl.program_id(0)
    come = jnp.where(side == 1 - core_index(), partner_ref[...], neighbor_ref[...])
    chunk = (own_ref[0].astype(F32) + come.astype(F32)).astype(BF16)
    full_ref[0] = chunk
    product = dot(chunk, probe_ref[...])

    @pl.when(side == 0)
    def _():
        acc[...] = inner_ref[...] + product

    @pl.when(side == 1)
    def _():
        acc[...] += product
        mine, other = halves(keep_ref.shape[0])
        keep_ref[...] = acc[mine, :].astype(BF16)
        give_ref[...] = acc[other, :].astype(BF16)


def pair_kernel(keep_ref, come_ref, out_ref):
    out_ref[...] = (keep_ref[...].astype(F32) + come_ref[...].astype(F32)).astype(BF16)


def add_kernel(start, count, *refs):
    rows = refs[-1].shape[0]
    cut = slice(start, start + rows)
    total = sum(ref[cut].astype(F32) for ref in refs[:count])
    for ref in refs[count:-1]:
        total += ref[...].astype(F32)
    refs[-1][...] = total.astype(BF16)


def total_kernel(parts_ref, out_ref):
    total = parts_ref[0].astype(F32)
    for i in range(1, parts_ref.shape[0]):
        total += parts_ref[i].astype(F32)
    total = total.astype(BF16)
    for i in range(out_ref.shape[0]):
        out_ref[i] = total


def split(value):
    high = value.astype(BF16)
    return high, (value - high.astype(F32)).astype(BF16)


def joined(both):
    return both[:, :BLK].astype(F32) + both[:, BLK:].astype(F32)


def pair_gram_kernel(keep_ref, come_ref, out_ref):
    half = keep_ref.shape[0] // 2
    for i in range(out_ref.shape[0]):
        rows = slice(8 * i, 8 * i + 8)
        out_ref[i, :8] = (keep_ref[rows].astype(F32) + come_ref[rows].astype(F32)).astype(BF16)
        rows = slice(half + 8 * i, half + 8 * i + 8)
        out_ref[i, 8:, :BLK], out_ref[i, 8:, BLK:] = split(joined(keep_ref[rows]) + joined(come_ref[rows]))


def total_gram_kernel(parts_ref, out_ref):
    total = parts_ref[0].astype(F32)
    for i in range(1, parts_ref.shape[0]):
        total += parts_ref[i].astype(F32)
    rows = total[:8].astype(BF16)
    high, low = split(total[8:, :BLK] + total[8:, BLK:])
    for i in range(out_ref.shape[0]):
        out_ref[i, :8] = rows
        out_ref[i, 8:, :BLK] = high
        out_ref[i, 8:, BLK:] = low


def in_order(mine_ref, other_ref, out):
    for part, rows in zip((mine_ref, other_ref), halves(mine_ref.shape[0])):
        out[rows, :] = part[...]


def half_of(role):
    core = core_index()
    return role + core - 2 * role * core


def sample_kernel(ranks, full_ref, mine_ref, other_ref, *refs):
    outs, fwd = refs[:-1], refs[-1]
    in_order(mine_ref, other_ref, fwd)
    for rel in range(ranks):
        owner = lax.rem(lax.axis_index("obs") + rel, ranks)
        for half in range(2):
            outs[2 * rel + half][...] = dot_tn(full_ref[2 * owner + half_of(half)], fwd[...]).astype(BF16)


def pick_kernel(ranks, *refs):
    pieces, out_ref = refs[:-1], refs[-1]
    rel = lax.rem(core_index() * (ranks - 1) + ranks - lax.axis_index("obs"), ranks)
    for i in range(ranks):

        @pl.when(rel == i)
        def _():
            rows = pieces[2 * i].shape[0]
            out_ref[:rows] = pieces[2 * i][...]
            out_ref[rows:] = pieces[2 * i + 1][...]


def project_kernel(ranks, full_ref, *refs):
    pieces = refs[: 3 * ranks]
    sample_ref, keep_ref, give_ref, acc, gram = refs[3 * ranks :]
    rows = pieces[2].shape[0]
    total = jnp.zeros(acc.shape, F32)
    square = jnp.zeros(gram.shape, F32)
    for rel in range(ranks):
        owner = lax.rem(lax.axis_index("obs") + rel, ranks)
        for half in range(2):
            parts = pieces[3 * rel : 3 * rel + 2] if half == 0 else pieces[3 * rel + 2 : 3 * rel + 3]
            piece = jnp.concatenate([part[...] for part in parts], axis=0)
            chunk = 2 * owner + half_of(half)
            sample_ref[pl.ds(pl.multiple_of(chunk * rows, rows), rows), :] = piece
            total += dot(full_ref[chunk], piece)
            square += dot_tn(piece, piece)
    acc[...] = total
    gram[...] = square
    rows = acc.shape[0] // 2
    for out_ref, mine in zip((keep_ref, give_ref), halves(rows)):
        out_ref[:rows] = acc[mine, :].astype(BF16)
    for out_ref, mine in zip((keep_ref, give_ref), halves(BLK)):
        out_ref[rows : 2 * rows, :BLK], out_ref[rows : 2 * rows, BLK:] = split(gram[:, mine])
    core = core_index()
    last = sample_ref.shape[0] - EDGE
    give_ref[2 * rows :] = sample_ref[pl.ds(pl.multiple_of((1 - core) * last, EDGE), EDGE), :]


def prior_block(block, off_ref, coefs, ext, base):
    total = dot(coefs[0], ext[pl.ds(pl.multiple_of(base + block * BLK, BLK), BLK), :])
    for j in range(2):
        start = base + (block + off_ref[j, block]) * BLK
        total += dot(coefs[j + 1], ext[pl.ds(pl.multiple_of(start, BLK), BLK), :])
    return total.astype(BF16)


def fill_ends(sample_ref, come_ref, neighbor_ref, ext):
    rows = sample_ref.shape[0]
    core = core_index()
    ext[EDGE : 3 * EDGE] = sample_ref[: 2 * EDGE]
    ext[3 * EDGE : 5 * EDGE] = sample_ref[rows - 2 * EDGE :]
    ext[pl.ds(pl.multiple_of((1 - core) * (5 * EDGE), EDGE), EDGE)] = come_ref[come_ref.shape[0] - EDGE :]
    ext[pl.ds(pl.multiple_of(core * (5 * EDGE), EDGE), EDGE)] = neighbor_ref[...]


def packed(full):
    return jnp.concatenate(
        [
            full[:NB, : 2 * NB],
            full[:NB, 2 * NB :],
            full[NB : 2 * NB, NB : 3 * NB],
            full[2 * NB : 3 * NB, 2 * NB :],
            jnp.concatenate([full[NB : 2 * NB, 3 * NB :], full[3 * NB :, 3 * NB :]], axis=1),
        ],
        axis=0,
    )


def unpacked(pack):
    r = [pack[i * NB : (i + 1) * NB] for i in range(5)]
    zero = jnp.zeros((NB, NB), F32)
    lane = lax.broadcasted_iota(jnp.int32, (NB, 2 * NB), 1)
    head = lambda block: jnp.where(lane < NB, 0.5, 1.0) * block
    join = lambda *p: jnp.concatenate(p, axis=1)
    return jnp.concatenate(
        [
            join(head(r[0]), r[1]),
            join(zero, head(r[2]), r[4][:, :NB]),
            join(zero, zero, head(r[3])),
            join(zero, zero, zero, 0.5 * r[4][:, NB:]),
        ],
        axis=0,
    )


def moments_kernel(mine_ref, other_ref, gram_ref, second_ref, proj):
    count = mine_ref.shape[0]
    for part, core in ((mine_ref, core_index()), (other_ref, 1 - core_index())):
        columns = pl.ds(pl.multiple_of(core * BLK, BLK), BLK)
        for i in range(count):
            proj[pl.ds(pl.multiple_of(core * (8 * count) + 8 * i, 8), 8), :] = part[i, :8].astype(F32)
            gram_ref[8 * i : 8 * i + 8, columns] = joined(part[i, 8:])
    rounded = proj[...].astype(BF16)
    second_ref[...] = packed(dot_tn(rounded, rounded)).astype(BF16)


def row_of(tile, k):
    return jnp.broadcast_to(tile[k : k + 1, :], tile.shape)


def lane_of(tile, k):
    return jnp.broadcast_to(tile[:, k : k + 1], (8, 2 * NB))


def factor_inverse(block):
    index = [lax.broadcasted_iota(jnp.int32, (NB, NB), d) for d in (0, 1)]
    wide = jnp.concatenate([block, (index[0] == index[1]).astype(F32)], axis=1)
    groups = NB // 8
    tiles = [wide[8 * t : 8 * t + 8] for t in range(groups)]
    row = lax.broadcasted_iota(jnp.int32, (8, 2 * NB), 0)
    out = []
    for g in range(groups):
        cols = {t: [lane_of(tiles[t], 8 * g + k) for k in range(8)] for t in range(g, groups)}
        done = tiles[g]
        for k in range(0, 8, 2):
            here = cols[g]
            p, q, r = row_of(here[k], k), row_of(here[k + 1], k), row_of(here[k + 1], k + 1)
            root = lax.rsqrt(p * r - q * q)
            inverse = root * root
            p_root = lax.rsqrt(p)
            row0, row1 = row_of(tiles[g], k), row_of(tiles[g], k + 1)
            second = (p * p_root * root) * (row1 - (q * p_root * p_root) * row0)
            done = jnp.where(row == k, p_root * row0, jnp.where(row == k + 1, second, done))
            head0 = [row_of(here[j], k) for j in range(k + 2, 8)]
            head1 = [row_of(here[j], k + 1) for j in range(k + 2, 8)]
            for t in range(g, groups):
                c0, c1 = cols[t][k], cols[t][k + 1]
                w0 = r * c0 - q * c1
                w1 = p * c1 - q * c0
                for j in range(k + 2, 8):
                    cols[t][j] = cols[t][j] - inverse * (w0 * head0[j - k - 2] + w1 * head1[j - k - 2])
                change = inverse * (w0 * row0 + w1 * row1)
                if t == g:
                    change = jnp.where(row > k + 1, change, 0.0)
                tiles[t] = tiles[t] - change
        out.append(done)
    return jnp.concatenate(out, axis=0)[:, NB:]


def exact(a, b, nt=False):
    return dot_nt(a, b, HI) if nt else jnp.dot(a, b, precision=HI, preferred_element_type=F32)


def factor_kernel(
    scale, gram_ref, off_ref, coef_ref, sample_ref, come_ref, neighbor_ref, out_ref, image_ref, a_ref, m_ref, inv_ref, ext
):
    n = out_ref.shape[0]
    count, rows = coef_ref.shape[0], sample_ref.shape[0]
    share = count * NB // n
    fill_ends(sample_ref, come_ref, neighbor_ref, ext)
    gram = gram_ref[...] * scale
    index = [lax.broadcasted_iota(jnp.int32, (n, n), d) for d in (0, 1)]
    diagonal = jnp.where(index[0] == index[1], gram, 0.0)
    across = lax.rsqrt(jnp.sum(diagonal, axis=0, keepdims=True))
    a_ref[...] = gram * across * lax.rsqrt(jnp.sum(diagonal, axis=1, keepdims=True))
    m_ref[...] = jnp.zeros((n, n), F32)
    inv_ref[...] = jnp.zeros((n, n), F32)
    for lo in range(0, n, NB):
        hi, nx = lo + NB, lo + 2 * NB
        inverse = factor_inverse(a_ref[lo:hi, lo:hi])
        inv_ref[lo:hi, lo:hi] = inverse
        first = lo // NB * share
        for block in range(first, first + share):
            coefs = [coef_ref[block, j] for j in range(3)]
            source, base = sample_ref, 0
            if block < REACH:
                source, base = ext, EDGE
            elif block >= count - REACH:
                source, base = ext, 5 * EDGE - rows
            image_ref[block * BLK : (block + 1) * BLK] = prior_block(block, off_ref, coefs, source, base)
        if hi < n:
            upper = exact(inverse, a_ref[lo:hi, hi:])
            lower = exact(a_ref[hi:, lo:hi], inverse, nt=True)
            a_ref[hi:nx, hi:nx] -= exact(lower[:NB], upper[:, :NB])
            if nx < n:
                a_ref[hi:nx, nx:] -= exact(lower[:NB], upper[:, NB:])
                a_ref[nx:, hi:] -= exact(lower[NB:], upper)
        if lo:
            inv_ref[lo:hi, :lo] = exact(inverse, m_ref[lo:hi, :lo])
        if hi < n:
            m_ref[hi:, :hi] -= exact(lower, inv_ref[lo:hi, :hi])
    out_ref[...] = (inv_ref[...] * across).astype(BF16)


def final_kernel(scale, inv_ref, rows_ref, sample_ref, image_ref, *refs):
    seconds, (basis_ref, mapped_ref, ritz_ref) = refs[:-3], refs[-3:]
    inverse = inv_ref[...]
    basis_ref[...] = dot_nt(sample_ref[...], inverse).astype(BF16)
    mapped_ref[...] = dot_nt(image_ref[...], inverse).astype(BF16)
    total = seconds[0][...].astype(F32)
    for part in seconds[1:]:
        total += part[...].astype(F32)
    upper = unpacked(total).astype(BF16)
    left = dot(rows_ref[...], upper) + dot_nt(rows_ref[...], upper)
    ritz_ref[...] = dot_nt(left.astype(BF16), inverse) * scale


def shifted(value, axis, by):
    count = lax.axis_size(axis)
    return lax.ppermute(value, axis, [(i, (i + by) % count) for i in range(count)])


def to_neighbor(value):
    count = lax.axis_size("par")
    pairs = [pair for i in range(1, count - 1, 2) for pair in ((i, i + 1), (i + 1, i))]
    return lax.ppermute(value, "par", pairs)


def swapped(value):
    return lax.ppermute(value, "par", [(i, i ^ 1) for i in range(lax.axis_size("par"))])


def exchanged(parts):
    groups = [[2 * i + core for i in range(parts.shape[0])] for core in range(2)]
    return lax.all_to_all(parts, "par", 0, 0, axis_index_groups=groups, tiled=True)


def body(jacobian, probes, coeffs, offsets):
    ranks = lax.axis_size("obs")
    chips = lax.axis_size("par") // 2
    nobs, npar = jacobian.shape[0], jacobian.shape[1]
    width = probes.shape[1]
    count = coeffs.shape[0]
    offsets = offsets.T
    flops = 2 * nobs * npar * width

    whole = lambda *dims: pl.BlockSpec(dims, lambda i: (0,) * len(dims))
    chunks = npar // EDGE
    last = chunks - 1
    partner, neighbor = pl.pallas_call(
        functools.partial(edges_kernel, count),
        name="edges",
        grid=(2,),
        out_shape=[shape(nobs, EDGE)] * 2,
        in_specs=[
            SMEM,
            pl.BlockSpec((nobs, EDGE), lambda i: (0, i * last)),
            pl.BlockSpec((REACH, *coeffs.shape[1:]), lambda i: (i * last, 0, 0, 0)),
        ],
        out_specs=[whole(nobs, EDGE)] * 2,
        scratch_shapes=[pltpu.VMEM((REACH, nobs, BLK), F32)],
        compiler_params=pltpu.CompilerParams(vmem_limit_bytes=50 * 2**20),
        cost_estimate=pl.CostEstimate(flops=flops // 4, bytes_accessed=0, transcendentals=0),
    )(offsets, jacobian, coeffs)
    from_neighbor = to_neighbor(neighbor)
    from_partner = swapped(partner)
    own = call(
        own_kernel,
        shape(chunks, nobs, EDGE),
        [SMEM, VMEM, VMEM],
        [offsets, jacobian, coeffs],
        [pltpu.VMEM((count + 2 * REACH, nobs, BLK), F32)],
        flops=4 * flops,
    )
    half = shape(nobs // 2, width)
    inner = call(inner_kernel, shape(nobs, width, dtype=F32), [VMEM] * 2, [own, probes], flops=flops)
    edge_chunk = pl.BlockSpec((1, nobs, EDGE), lambda i: (i * last, 0, 0))
    full, keep, give = pl.pallas_call(
        forward_kernel,
        name="forward",
        grid=(2,),
        out_shape=[shape(chunks, nobs, EDGE), half, half],
        in_specs=[
            edge_chunk,
            whole(nobs, EDGE),
            whole(nobs, EDGE),
            pl.BlockSpec((EDGE, width), lambda i: (i * last, 0)),
            whole(nobs, width),
        ],
        out_specs=[edge_chunk, whole(*half.shape), whole(*half.shape)],
        scratch_shapes=[pltpu.VMEM((nobs, width), F32)],
        input_output_aliases={0: 0},
        compiler_params=pltpu.CompilerParams(vmem_limit_bytes=24 * 2**20),
    )(own, from_partner, from_neighbor, probes, inner)
    part = call(pair_kernel, half, [VMEM] * 2, [keep, swapped(give)], mib=4)
    parts = exchanged(part.reshape(chips, nobs // 2 // chips, width))
    total = call(total_kernel, shape(*parts.shape), [VMEM], [parts], mib=4)
    mine = exchanged(total).reshape(half.shape)
    other = swapped(mine)

    pieces = call(
        functools.partial(sample_kernel, ranks),
        [shape(npar // ranks // 2, width)] * (2 * ranks),
        [VMEM] * 3,
        [full, mine, other],
        [pltpu.VMEM((nobs, width), BF16)],
        mib=16,
        flops=flops,
    )
    here0, here1, right0, right1, far0, far1, left0, left1 = pieces

    def ring(value, by):
        return shifted(value, "obs", by)

    def add(start, rows, whole, parts=()):
        kernel = functools.partial(add_kernel, start, len(whole))
        return call(kernel, shape(rows, width), [VMEM] * (len(whole) + len(parts)), [*whole, *parts], mib=4)

    via_left = ring(far0, 1)
    via_right = ring(far1, -1)
    own_up = ring(right1, 1)
    own_down = ring(left0, -1)
    rows = EDGE // 2
    sums_up = [ring(add(i * rows, rows, [right0, via_left]), 1) for i in range(2)]
    sum_down = ring(add(0, EDGE, [left1, via_right]), -1)
    sums0 = [add(i * rows, rows, [here0, own_down], [sums_up[i]]) for i in range(2)]
    sum1 = add(0, EDGE, [here1, own_up, sum_down])
    l0 = [ring(sums0[i], 1) for i in range(2)]
    r0 = [ring(sums0[i], -1) for i in range(2)]
    f0 = [ring(l0[i], 1) for i in range(2)]
    l1 = ring(sum1, 1)
    r1 = ring(sum1, -1)
    f1 = ring(r1, -1)

    neighbor = call(
        functools.partial(pick_kernel, ranks), shape(EDGE, width), [VMEM] * (2 * ranks), [*sums0, *r0, *f0, *l0], mib=4
    )
    from_neighbor = to_neighbor(neighbor)
    sample, keep, give = call(
        functools.partial(project_kernel, ranks),
        [shape(npar, width), shape(nobs, width), shape(nobs + EDGE, width)],
        [VMEM] * (1 + 3 * ranks),
        [full, *sums0, sum1, *r0, r1, *f0, f1, *l0, l1],
        [pltpu.VMEM((nobs, width), F32), pltpu.VMEM((width, width), F32)],
        mib=16,
        flops=flops,
    )
    come = swapped(give)
    both = shape(chips, 16, width)
    part = call(pair_gram_kernel, both, [VMEM] * 2, [keep, come], mib=4)
    total = call(total_gram_kernel, both, [VMEM], [exchanged(part)], mib=4)
    mine = exchanged(total)
    other = swapped(mine)
    gram, second = call(
        moments_kernel,
        [shape(width, width, dtype=F32), shape(5 * NB, 2 * NB)],
        [VMEM] * 2,
        [mine, other],
        [pltpu.VMEM((nobs, width), F32)],
        mib=8,
        flops=flops // 8,
    )
    seconds = [second] + [shifted(second, "obs", by) for by in (1, -1, 2)]
    total_par = npar * lax.axis_size("par")
    inverse, image = call(
        functools.partial(factor_kernel, 1.0 / total_par),
        [shape(width, width), shape(npar, width)],
        [VMEM, SMEM] + [VMEM] * 4,
        [gram, offsets, coeffs, sample, come, from_neighbor],
        [pltpu.VMEM((width, width), F32)] * 3 + [pltpu.VMEM((6 * EDGE, width), BF16)],
        mib=16,
        flops=16 * flops,
    )
    steps = 4
    by_rows = pl.BlockSpec((npar // steps, width), lambda i: (i, 0))
    few = pl.BlockSpec((width // steps, width), lambda i: (i, 0))
    return pl.pallas_call(
        functools.partial(final_kernel, 1.0 / (nobs * ranks)),
        name="final",
        grid=(steps,),
        out_shape=[shape(npar, width), shape(npar, width), shape(width, width, dtype=F32)],
        in_specs=[whole(width, width), few, by_rows, by_rows] + [whole(*second.shape)] * len(seconds),
        out_specs=[by_rows, by_rows, few],
        compiler_params=pltpu.CompilerParams(vmem_limit_bytes=12 * 2**20),
    )(inverse, inverse, sample, image, *seconds)


def solution(mesh):
    return jax.shard_map(
        body,
        mesh=mesh,
        in_specs=(P("obs", "par"), P("par", None), P("par", None, None, None), P("par", None)),
        out_specs=(P("par", None), P("par", None), P()),
        check_vma=False,
    )
```

```python
import functools

import jax
import jax.numpy as jnp
from jax import lax
from jax.experimental import pallas as pl
from jax.experimental.pallas import tpu as pltpu
from jax.sharding import PartitionSpec as P


BLK = 128
REACH = 4
EDGE = REACH * BLK
NB = 64
F32 = jnp.float32
BF16 = jnp.bfloat16
HI = lax.Precision.HIGHEST
VMEM = pl.BlockSpec(memory_space=pltpu.VMEM)
SMEM = pl.BlockSpec(memory_space=pltpu.SMEM)


def core_index():
    return lax.rem(lax.axis_index("par"), 2)


def call(kernel, outs, specs, args, scratch=(), mib=24, flops=0):
    return pl.pallas_call(
        kernel,
        out_shape=outs,
        in_specs=specs,
        out_specs=jax.tree.map(lambda _: VMEM, outs),
        scratch_shapes=scratch,
        compiler_params=pltpu.CompilerParams(vmem_limit_bytes=mib * 2**20),
        cost_estimate=pl.CostEstimate(flops=flops, bytes_accessed=0, transcendentals=0),
    )(*args)


def dot(a, b):
    return jnp.dot(a, b, preferred_element_type=F32)


def dot_tn(a, b, precision=None):
    return lax.dot_general(a, b, (((0,), (0,)), ((), ())), precision=precision, preferred_element_type=F32)


def dot_nt(a, b, precision=None):
    return lax.dot_general(a, b, (((1,), (1,)), ((), ())), precision=precision, preferred_element_type=F32)


def shape(*dims, dtype=BF16):
    return jax.ShapeDtypeStruct(dims, dtype)


def edges_kernel(count, off_ref, jac_ref, coef_ref, partner_ref, neighbor_ref, acc):
    side = pl.program_id(0)
    acc[...] = jnp.zeros_like(acc)
    for i in range(REACH):
        block = i + side * (count - REACH)
        columns = jac_ref[:, i * BLK : (i + 1) * BLK]
        for j in range(2):
            target = block + off_ref[j, block]
            place = jnp.where(side == 0, target + REACH, target - count)

            @pl.when((place >= 0) & (place < REACH))
            def _():
                acc[place] += dot(columns, coef_ref[i, j + 1])

    for out_ref, wanted in ((partner_ref, 1 - core_index()), (neighbor_ref, core_index())):

        @pl.when(side == wanted)
        def _():
            for i in range(REACH):
                out_ref[:, i * BLK : (i + 1) * BLK] = acc[i].astype(BF16)


def own_kernel(off_ref, jac_ref, coef_ref, out_ref, acc):
    count = coef_ref.shape[0]
    for i in range(REACH):
        acc[i] = jnp.zeros_like(acc[i])
        acc[count + REACH + i] = jnp.zeros_like(acc[i])

    def diagonal(block, carry):
        columns = jac_ref[:, pl.ds(pl.multiple_of(block * BLK, BLK), BLK)]
        acc[block + REACH] = dot(columns, coef_ref[block, 0])
        return carry

    lax.fori_loop(0, count, diagonal, 0, unroll=8)

    def band(block, carry):
        columns = jac_ref[:, pl.ds(pl.multiple_of(block * BLK, BLK), BLK)]
        for j in range(2):
            acc[block + REACH + off_ref[j, block]] += dot(columns, coef_ref[block, j + 1])
        return carry

    lax.fori_loop(0, count, band, 0, unroll=8)
    for block in range(count):
        place = block % REACH
        out_ref[block // REACH, :, place * BLK : (place + 1) * BLK] = acc[block + REACH].astype(BF16)


def inner_kernel(own_ref, probe_ref, out_ref):
    chunks = own_ref.shape[0]
    out_ref[...] = sum(dot(own_ref[i], probe_ref[i * EDGE : (i + 1) * EDGE, :]) for i in range(1, chunks - 1))


def halves(rows):
    core = core_index()
    return [pl.ds(pl.multiple_of(i * rows, rows), rows) for i in (core, 1 - core)]


def forward_kernel(own_ref, partner_ref, neighbor_ref, probe_ref, inner_ref, full_ref, keep_ref, give_ref, acc):
    side = pl.program_id(0)
    come = jnp.where(side == 1 - core_index(), partner_ref[...], neighbor_ref[...])
    chunk = (own_ref[0].astype(F32) + come.astype(F32)).astype(BF16)
    full_ref[0] = chunk
    product = dot(chunk, probe_ref[...])

    @pl.when(side == 0)
    def _():
        acc[...] = inner_ref[...] + product

    @pl.when(side == 1)
    def _():
        acc[...] += product
        mine, other = halves(keep_ref.shape[0])
        keep_ref[...] = acc[mine, :].astype(BF16)
        give_ref[...] = acc[other, :].astype(BF16)


def pair_kernel(keep_ref, come_ref, out_ref):
    out_ref[...] = (keep_ref[...].astype(F32) + come_ref[...].astype(F32)).astype(BF16)


def add_kernel(start, count, *refs):
    rows = refs[-1].shape[0]
    cut = slice(start, start + rows)
    total = sum(ref[cut].astype(F32) for ref in refs[:count])
    for ref in refs[count:-1]:
        total += ref[...].astype(F32)
    refs[-1][...] = total.astype(BF16)


def total_kernel(parts_ref, out_ref):
    total = parts_ref[0].astype(F32)
    for i in range(1, parts_ref.shape[0]):
        total += parts_ref[i].astype(F32)
    total = total.astype(BF16)
    for i in range(out_ref.shape[0]):
        out_ref[i] = total


def split(value):
    high = value.astype(BF16)
    return high, (value - high.astype(F32)).astype(BF16)


def joined(both):
    return both[:, :BLK].astype(F32) + both[:, BLK:].astype(F32)


def pair_gram_kernel(keep_ref, come_ref, out_ref):
    half = keep_ref.shape[0] // 2
    for i in range(out_ref.shape[0]):
        rows = slice(8 * i, 8 * i + 8)
        out_ref[i, :8] = (keep_ref[rows].astype(F32) + come_ref[rows].astype(F32)).astype(BF16)
        rows = slice(half + 8 * i, half + 8 * i + 8)
        out_ref[i, 8:, :BLK], out_ref[i, 8:, BLK:] = split(joined(keep_ref[rows]) + joined(come_ref[rows]))


def total_gram_kernel(parts_ref, out_ref):
    total = parts_ref[0].astype(F32)
    for i in range(1, parts_ref.shape[0]):
        total += parts_ref[i].astype(F32)
    rows = total[:8].astype(BF16)
    high, low = split(total[8:, :BLK] + total[8:, BLK:])
    for i in range(out_ref.shape[0]):
        out_ref[i, :8] = rows
        out_ref[i, 8:, :BLK] = high
        out_ref[i, 8:, BLK:] = low


def in_order(mine_ref, other_ref, out):
    for part, rows in zip((mine_ref, other_ref), halves(mine_ref.shape[0])):
        out[rows, :] = part[...]


def half_of(role):
    core = core_index()
    return role + core - 2 * role * core


def sample_kernel(ranks, full_ref, mine_ref, other_ref, *refs):
    outs, fwd = refs[:-1], refs[-1]
    in_order(mine_ref, other_ref, fwd)
    for rel in range(ranks):
        owner = lax.rem(lax.axis_index("obs") + rel, ranks)
        for half in range(2):
            outs[2 * rel + half][...] = dot_tn(full_ref[2 * owner + half_of(half)], fwd[...]).astype(BF16)


def pick_kernel(ranks, *refs):
    pieces, out_ref = refs[:-1], refs[-1]
    rel = lax.rem(core_index() * (ranks - 1) + ranks - lax.axis_index("obs"), ranks)
    for i in range(ranks):

        @pl.when(rel == i)
        def _():
            rows = pieces[2 * i].shape[0]
            out_ref[:rows] = pieces[2 * i][...]
            out_ref[rows:] = pieces[2 * i + 1][...]


def project_kernel(ranks, full_ref, passed_ref, *refs):
    pieces = refs[: 3 * ranks]
    sample_ref, keep_ref, give_ref, acc, gram = refs[3 * ranks :]
    rows = pieces[2].shape[0]
    total = jnp.zeros(acc.shape, F32)
    square = jnp.zeros(gram.shape, F32)
    for rel in range(ranks):
        owner = lax.rem(lax.axis_index("obs") + rel, ranks)
        for half in range(2):
            parts = pieces[3 * rel : 3 * rel + 2] if half == 0 else pieces[3 * rel + 2 : 3 * rel + 3]
            piece = jnp.concatenate([part[...] for part in parts], axis=0)
            chunk = 2 * owner + half_of(half)
            sample_ref[pl.ds(pl.multiple_of(chunk * rows, rows), rows), :] = piece
            total += dot(full_ref[chunk], piece)
            square += dot_tn(piece, piece)
    acc[...] = total
    gram[...] = square
    rows = acc.shape[0] // 2
    for out_ref, mine in zip((keep_ref, give_ref), halves(rows)):
        out_ref[:rows] = acc[mine, :].astype(BF16)
    for out_ref, mine in zip((keep_ref, give_ref), halves(BLK)):
        out_ref[rows : 2 * rows, :BLK], out_ref[rows : 2 * rows, BLK:] = split(gram[:, mine])
    core = core_index()
    last = sample_ref.shape[0] - EDGE
    give_ref[2 * rows + EDGE :] = passed_ref[...]
    give_ref[2 * rows : 2 * rows + EDGE] = sample_ref[pl.ds(pl.multiple_of((1 - core) * last, EDGE), EDGE), :]


def prior_block(block, off_ref, coefs, ext, base):
    total = dot(coefs[0], ext[pl.ds(pl.multiple_of(base + block * BLK, BLK), BLK), :])
    for j in range(2):
        start = base + (block + off_ref[j, block]) * BLK
        total += dot(coefs[j + 1], ext[pl.ds(pl.multiple_of(start, BLK), BLK), :])
    return total.astype(BF16)


def fill_ends(sample_ref, come_ref, neighbor_ref, ext):
    rows = sample_ref.shape[0]
    core = core_index()
    ext[EDGE : 3 * EDGE] = sample_ref[: 2 * EDGE]
    ext[3 * EDGE : 5 * EDGE] = sample_ref[rows - 2 * EDGE :]
    near = come_ref.shape[0] - 2 * EDGE
    ext[pl.ds(pl.multiple_of((1 - core) * (5 * EDGE), EDGE), EDGE)] = come_ref[near : near + EDGE]
    far = jnp.where(core == 0, come_ref[near + EDGE :], neighbor_ref[...])
    ext[pl.ds(pl.multiple_of(core * (5 * EDGE), EDGE), EDGE)] = far


def packed(full):
    return jnp.concatenate(
        [
            full[:NB, : 2 * NB],
            full[:NB, 2 * NB :],
            full[NB : 2 * NB, NB : 3 * NB],
            full[2 * NB : 3 * NB, 2 * NB :],
            jnp.concatenate([full[NB : 2 * NB, 3 * NB :], full[3 * NB :, 3 * NB :]], axis=1),
        ],
        axis=0,
    )


def unpacked(pack):
    r = [pack[i * NB : (i + 1) * NB] for i in range(5)]
    zero = jnp.zeros((NB, NB), F32)
    lane = lax.broadcasted_iota(jnp.int32, (NB, 2 * NB), 1)
    head = lambda block: jnp.where(lane < NB, 0.5, 1.0) * block
    join = lambda *p: jnp.concatenate(p, axis=1)
    return jnp.concatenate(
        [
            join(head(r[0]), r[1]),
            join(zero, head(r[2]), r[4][:, :NB]),
            join(zero, zero, head(r[3])),
            join(zero, zero, zero, 0.5 * r[4][:, NB:]),
        ],
        axis=0,
    )


def moments_kernel(mine_ref, other_ref, gram_ref, second_ref, proj):
    count = mine_ref.shape[0]
    for part, core in ((mine_ref, core_index()), (other_ref, 1 - core_index())):
        columns = pl.ds(pl.multiple_of(core * BLK, BLK), BLK)
        for i in range(count):
            proj[pl.ds(pl.multiple_of(core * (8 * count) + 8 * i, 8), 8), :] = part[i, :8].astype(F32)
            gram_ref[8 * i : 8 * i + 8, columns] = joined(part[i, 8:])
    rounded = proj[...].astype(BF16)
    second_ref[...] = packed(dot_tn(rounded, rounded)).astype(BF16)


def row_of(tile, k):
    return jnp.broadcast_to(tile[k : k + 1, :], tile.shape)


def lane_of(tile, k):
    return jnp.broadcast_to(tile[:, k : k + 1], (8, 2 * NB))


def factor_inverse(block):
    index = [lax.broadcasted_iota(jnp.int32, (NB, NB), d) for d in (0, 1)]
    wide = jnp.concatenate([block, (index[0] == index[1]).astype(F32)], axis=1)
    groups = NB // 8
    tiles = [wide[8 * t : 8 * t + 8] for t in range(groups)]
    row = lax.broadcasted_iota(jnp.int32, (8, 2 * NB), 0)
    out = []
    for g in range(groups):
        cols = {t: [lane_of(tiles[t], 8 * g + k) for k in range(8)] for t in range(g, groups)}
        done = tiles[g]
        for k in range(0, 8, 2):
            here = cols[g]
            p, q, r = row_of(here[k], k), row_of(here[k + 1], k), row_of(here[k + 1], k + 1)
            root = lax.rsqrt(p * r - q * q)
            inverse = root * root
            p_root = lax.rsqrt(p)
            row0, row1 = row_of(tiles[g], k), row_of(tiles[g], k + 1)
            second = (p * p_root * root) * (row1 - (q * p_root * p_root) * row0)
            done = jnp.where(row == k, p_root * row0, jnp.where(row == k + 1, second, done))
            head0 = [row_of(here[j], k) for j in range(k + 2, 8)]
            head1 = [row_of(here[j], k + 1) for j in range(k + 2, 8)]
            for t in range(g, groups):
                c0, c1 = cols[t][k], cols[t][k + 1]
                w0 = r * c0 - q * c1
                w1 = p * c1 - q * c0
                for j in range(k + 2, 8):
                    cols[t][j] = cols[t][j] - inverse * (w0 * head0[j - k - 2] + w1 * head1[j - k - 2])
                change = inverse * (w0 * row0 + w1 * row1)
                if t == g:
                    change = jnp.where(row > k + 1, change, 0.0)
                tiles[t] = tiles[t] - change
        out.append(done)
    return jnp.concatenate(out, axis=0)[:, NB:]


def exact(a, b, nt=False):
    return dot_nt(a, b, HI) if nt else jnp.dot(a, b, precision=HI, preferred_element_type=F32)


def factor_kernel(
    scale, gram_ref, off_ref, coef_ref, sample_ref, come_ref, neighbor_ref, out_ref, image_ref, a_ref, m_ref, inv_ref, ext
):
    n = out_ref.shape[0]
    count, rows = coef_ref.shape[0], sample_ref.shape[0]
    share = count * NB // n
    fill_ends(sample_ref, come_ref, neighbor_ref, ext)
    gram = gram_ref[...] * scale
    index = [lax.broadcasted_iota(jnp.int32, (n, n), d) for d in (0, 1)]
    diagonal = jnp.where(index[0] == index[1], gram, 0.0)
    across = lax.rsqrt(jnp.sum(diagonal, axis=0, keepdims=True))
    a_ref[...] = gram * across * lax.rsqrt(jnp.sum(diagonal, axis=1, keepdims=True))
    m_ref[...] = jnp.zeros((n, n), F32)
    inv_ref[...] = jnp.zeros((n, n), F32)
    for lo in range(0, n, NB):
        hi, nx = lo + NB, lo + 2 * NB
        inverse = factor_inverse(a_ref[lo:hi, lo:hi])
        inv_ref[lo:hi, lo:hi] = inverse
        first = lo // NB * share
        for block in range(first, first + share):
            coefs = [coef_ref[block, j] for j in range(3)]
            source, base = sample_ref, 0
            if block < REACH:
                source, base = ext, EDGE
            elif block >= count - REACH:
                source, base = ext, 5 * EDGE - rows
            image_ref[block * BLK : (block + 1) * BLK] = prior_block(block, off_ref, coefs, source, base)
        if hi < n:
            upper = exact(inverse, a_ref[lo:hi, hi:])
            lower = exact(a_ref[hi:, lo:hi], inverse, nt=True)
            a_ref[hi:nx, hi:nx] -= exact(lower[:NB], upper[:, :NB])
            if nx < n:
                a_ref[hi:nx, nx:] -= exact(lower[:NB], upper[:, NB:])
                a_ref[nx:, hi:] -= exact(lower[NB:], upper)
        if lo:
            inv_ref[lo:hi, :lo] = exact(inverse, m_ref[lo:hi, :lo])
        if hi < n:
            m_ref[hi:, :hi] -= exact(lower, inv_ref[lo:hi, :hi])
    out_ref[...] = (inv_ref[...] * across).astype(BF16)


def final_kernel(scale, inv_ref, rows_ref, sample_ref, image_ref, *refs):
    seconds, (basis_ref, mapped_ref, ritz_ref) = refs[:-3], refs[-3:]
    inverse = inv_ref[...]
    basis_ref[...] = dot_nt(sample_ref[...], inverse).astype(BF16)
    mapped_ref[...] = dot_nt(image_ref[...], inverse).astype(BF16)
    total = seconds[0][...].astype(F32)
    for part in seconds[1:]:
        total += part[...].astype(F32)
    upper = unpacked(total).astype(BF16)
    left = dot(rows_ref[...], upper) + dot_nt(rows_ref[...], upper)
    ritz_ref[...] = dot_nt(left.astype(BF16), inverse) * scale


def shifted(value, axis, by):
    count = lax.axis_size(axis)
    return lax.ppermute(value, axis, [(i, (i + by) % count) for i in range(count)])


def to_neighbor(value):
    count = lax.axis_size("par")
    pairs = [pair for i in range(1, count - 1, 2) for pair in ((i, i + 1), (i + 1, i))]
    return lax.ppermute(value, "par", pairs)


def swapped(value):
    return lax.ppermute(value, "par", [(i, i ^ 1) for i in range(lax.axis_size("par"))])


def exchanged(parts):
    groups = [[2 * i + core for i in range(parts.shape[0])] for core in range(2)]
    return lax.all_to_all(parts, "par", 0, 0, axis_index_groups=groups, tiled=True)


def body(jacobian, probes, coeffs, offsets):
    ranks = lax.axis_size("obs")
    chips = lax.axis_size("par") // 2
    nobs, npar = jacobian.shape[0], jacobian.shape[1]
    width = probes.shape[1]
    count = coeffs.shape[0]
    offsets = offsets.T
    flops = 2 * nobs * npar * width

    whole = lambda *dims: pl.BlockSpec(dims, lambda i: (0,) * len(dims))
    chunks = npar // EDGE
    last = chunks - 1
    partner, neighbor = pl.pallas_call(
        functools.partial(edges_kernel, count),
        name="edges",
        grid=(2,),
        out_shape=[shape(nobs, EDGE)] * 2,
        in_specs=[
            SMEM,
            pl.BlockSpec((nobs, EDGE), lambda i: (0, i * last)),
            pl.BlockSpec((REACH, *coeffs.shape[1:]), lambda i: (i * last, 0, 0, 0)),
        ],
        out_specs=[whole(nobs, EDGE)] * 2,
        scratch_shapes=[pltpu.VMEM((REACH, nobs, BLK), F32)],
        compiler_params=pltpu.CompilerParams(vmem_limit_bytes=50 * 2**20),
        cost_estimate=pl.CostEstimate(flops=flops // 4, bytes_accessed=0, transcendentals=0),
    )(offsets, jacobian, coeffs)
    from_neighbor = to_neighbor(neighbor)
    from_partner = swapped(partner)
    own = call(
        own_kernel,
        shape(chunks, nobs, EDGE),
        [SMEM, VMEM, VMEM],
        [offsets, jacobian, coeffs],
        [pltpu.VMEM((count + 2 * REACH, nobs, BLK), F32)],
        flops=4 * flops,
    )
    half = shape(nobs // 2, width)
    inner = call(inner_kernel, shape(nobs, width, dtype=F32), [VMEM] * 2, [own, probes], flops=flops)
    edge_chunk = pl.BlockSpec((1, nobs, EDGE), lambda i: (i * last, 0, 0))
    full, keep, give = pl.pallas_call(
        forward_kernel,
        name="forward",
        grid=(2,),
        out_shape=[shape(chunks, nobs, EDGE), half, half],
        in_specs=[
            edge_chunk,
            whole(nobs, EDGE),
            whole(nobs, EDGE),
            pl.BlockSpec((EDGE, width), lambda i: (i * last, 0)),
            whole(nobs, width),
        ],
        out_specs=[edge_chunk, whole(*half.shape), whole(*half.shape)],
        scratch_shapes=[pltpu.VMEM((nobs, width), F32)],
        input_output_aliases={0: 0},
        compiler_params=pltpu.CompilerParams(vmem_limit_bytes=24 * 2**20),
    )(own, from_partner, from_neighbor, probes, inner)
    part = call(pair_kernel, half, [VMEM] * 2, [keep, swapped(give)], mib=4)
    parts = exchanged(part.reshape(chips, nobs // 2 // chips, width))
    total = call(total_kernel, shape(*parts.shape), [VMEM], [parts], mib=4)
    mine = exchanged(total).reshape(half.shape)
    other = swapped(mine)

    pieces = call(
        functools.partial(sample_kernel, ranks),
        [shape(npar // ranks // 2, width)] * (2 * ranks),
        [VMEM] * 3,
        [full, mine, other],
        [pltpu.VMEM((nobs, width), BF16)],
        mib=16,
        flops=flops,
    )
    here0, here1, right0, right1, far0, far1, left0, left1 = pieces

    def ring(value, by):
        return shifted(value, "obs", by)

    def add(start, rows, whole, parts=()):
        kernel = functools.partial(add_kernel, start, len(whole))
        return call(kernel, shape(rows, width), [VMEM] * (len(whole) + len(parts)), [*whole, *parts], mib=4)

    via_left = ring(far0, 1)
    via_right = ring(far1, -1)
    own_up = ring(right1, 1)
    own_down = ring(left0, -1)
    rows = EDGE // 2
    sums_up = [ring(add(i * rows, rows, [right0, via_left]), 1) for i in range(2)]
    sum_down = ring(add(0, EDGE, [left1, via_right]), -1)
    sums0 = [add(i * rows, rows, [here0, own_down], [sums_up[i]]) for i in range(2)]
    sum1 = add(0, EDGE, [here1, own_up, sum_down])
    l0 = [ring(sums0[i], 1) for i in range(2)]
    r0 = [ring(sums0[i], -1) for i in range(2)]
    f0 = [ring(l0[i], 1) for i in range(2)]
    l1 = ring(sum1, 1)
    r1 = ring(sum1, -1)
    f1 = ring(r1, -1)

    neighbor = call(
        functools.partial(pick_kernel, ranks), shape(EDGE, width), [VMEM] * (2 * ranks), [*sums0, *r0, *f0, *l0], mib=4
    )
    cores = lax.axis_size("par")
    passed = lax.ppermute(neighbor, "par", [(i, i + 2) for i in range(1, cores - 2, 2)])
    from_neighbor = lax.ppermute(neighbor, "par", [(i, i - 1) for i in range(2, cores, 2)])
    sample, keep, give = call(
        functools.partial(project_kernel, ranks),
        [shape(npar, width), shape(nobs, width), shape(nobs + 2 * EDGE, width)],
        [VMEM] * (2 + 3 * ranks),
        [full, passed, *sums0, sum1, *r0, r1, *f0, f1, *l0, l1],
        [pltpu.VMEM((nobs, width), F32), pltpu.VMEM((width, width), F32)],
        mib=16,
        flops=flops,
    )
    come = swapped(give)
    both = shape(chips, 16, width)
    part = call(pair_gram_kernel, both, [VMEM] * 2, [keep, come], mib=4)
    total = call(total_gram_kernel, both, [VMEM], [exchanged(part)], mib=4)
    mine = exchanged(total)
    other = swapped(mine)
    gram, second = call(
        moments_kernel,
        [shape(width, width, dtype=F32), shape(5 * NB, 2 * NB)],
        [VMEM] * 2,
        [mine, other],
        [pltpu.VMEM((nobs, width), F32)],
        mib=8,
        flops=flops // 8,
    )
    seconds = [second] + [shifted(second, "obs", by) for by in (1, -1, 2)]
    total_par = npar * lax.axis_size("par")
    inverse, image = call(
        functools.partial(factor_kernel, 1.0 / total_par),
        [shape(width, width), shape(npar, width)],
        [VMEM, SMEM] + [VMEM] * 4,
        [gram, offsets, coeffs, sample, come, from_neighbor],
        [pltpu.VMEM((width, width), F32)] * 3 + [pltpu.VMEM((6 * EDGE, width), BF16)],
        mib=16,
        flops=16 * flops,
    )
    steps = 2
    by_rows = pl.BlockSpec((npar // steps, width), lambda i: (i, 0))
    few = pl.BlockSpec((width // steps, width), lambda i: (i, 0))
    return pl.pallas_call(
        functools.partial(final_kernel, 1.0 / (nobs * ranks)),
        name="final",
        grid=(steps,),
        out_shape=[shape(npar, width), shape(npar, width), shape(width, width, dtype=F32)],
        in_specs=[whole(width, width), few, by_rows, by_rows] + [whole(*second.shape)] * len(seconds),
        out_specs=[by_rows, by_rows, few],
        compiler_params=pltpu.CompilerParams(vmem_limit_bytes=16 * 2**20),
    )(inverse, inverse, sample, image, *seconds)


def solution(mesh):
    return jax.shard_map(
        body,
        mesh=mesh,
        in_specs=(P("obs", "par"), P("par", None), P("par", None, None, None), P("par", None)),
        out_specs=(P("par", None), P("par", None), P()),
        check_vma=False,
    )
```

```python
import functools

import jax
import jax.numpy as jnp
from jax import lax
from jax.experimental import pallas as pl
from jax.experimental.pallas import tpu as pltpu
from jax.sharding import PartitionSpec as P


BLK = 128
REACH = 4
EDGE = REACH * BLK
NB = 64
F32 = jnp.float32
BF16 = jnp.bfloat16
HI = lax.Precision.HIGHEST
VMEM = pl.BlockSpec(memory_space=pltpu.VMEM)
SMEM = pl.BlockSpec(memory_space=pltpu.SMEM)


def core_index():
    return lax.rem(lax.axis_index("par"), 2)


def call(kernel, outs, specs, args, scratch=(), mib=24, flops=0):
    return pl.pallas_call(
        kernel,
        out_shape=outs,
        in_specs=specs,
        out_specs=jax.tree.map(lambda _: VMEM, outs),
        scratch_shapes=scratch,
        compiler_params=pltpu.CompilerParams(vmem_limit_bytes=mib * 2**20),
        cost_estimate=pl.CostEstimate(flops=flops, bytes_accessed=0, transcendentals=0),
    )(*args)


def dot(a, b):
    return jnp.dot(a, b, preferred_element_type=F32)


def dot_tn(a, b, precision=None):
    return lax.dot_general(a, b, (((0,), (0,)), ((), ())), precision=precision, preferred_element_type=F32)


def dot_nt(a, b, precision=None):
    return lax.dot_general(a, b, (((1,), (1,)), ((), ())), precision=precision, preferred_element_type=F32)


def shape(*dims, dtype=BF16):
    return jax.ShapeDtypeStruct(dims, dtype)


def edges_kernel(count, off_ref, jac_ref, coef_ref, partner_ref, neighbor_ref, acc):
    side = pl.program_id(0)
    acc[...] = jnp.zeros_like(acc)
    for i in range(REACH):
        block = i + side * (count - REACH)
        columns = jac_ref[:, i * BLK : (i + 1) * BLK]
        for j in range(2):
            target = block + off_ref[j, block]
            place = jnp.where(side == 0, target + REACH, target - count)

            @pl.when((place >= 0) & (place < REACH))
            def _():
                acc[place] += dot(columns, coef_ref[i, j + 1])

    for out_ref, wanted in ((partner_ref, 1 - core_index()), (neighbor_ref, core_index())):

        @pl.when(side == wanted)
        def _():
            for i in range(REACH):
                out_ref[:, i * BLK : (i + 1) * BLK] = acc[i].astype(BF16)


def own_kernel(off_ref, jac_ref, coef_ref, out_ref, acc):
    count = coef_ref.shape[0]
    for i in range(REACH):
        acc[i] = jnp.zeros_like(acc[i])
        acc[count + REACH + i] = jnp.zeros_like(acc[i])

    def diagonal(block, carry):
        columns = jac_ref[:, pl.ds(pl.multiple_of(block * BLK, BLK), BLK)]
        acc[block + REACH] = dot(columns, coef_ref[block, 0])
        return carry

    lax.fori_loop(0, count, diagonal, 0, unroll=8)

    def band(block, carry):
        columns = jac_ref[:, pl.ds(pl.multiple_of(block * BLK, BLK), BLK)]
        for j in range(2):
            acc[block + REACH + off_ref[j, block]] += dot(columns, coef_ref[block, j + 1])
        return carry

    lax.fori_loop(0, count, band, 0, unroll=8)
    for block in range(count):
        place = block % REACH
        out_ref[block // REACH, :, place * BLK : (place + 1) * BLK] = acc[block + REACH].astype(BF16)


def inner_kernel(own_ref, probe_ref, out_ref):
    chunks = own_ref.shape[0]
    out_ref[...] = sum(dot(own_ref[i], probe_ref[i * EDGE : (i + 1) * EDGE, :]) for i in range(1, chunks - 1))


def halves(rows):
    core = core_index()
    return [pl.ds(pl.multiple_of(i * rows, rows), rows) for i in (core, 1 - core)]


def forward_kernel(own_ref, partner_ref, neighbor_ref, probe_ref, inner_ref, full_ref, keep_ref, give_ref, acc):
    side = pl.program_id(0)
    come = jnp.where(side == 1 - core_index(), partner_ref[...], neighbor_ref[...])
    chunk = (own_ref[0].astype(F32) + come.astype(F32)).astype(BF16)
    full_ref[0] = chunk
    product = dot(chunk, probe_ref[...])

    @pl.when(side == 0)
    def _():
        acc[...] = inner_ref[...] + product

    @pl.when(side == 1)
    def _():
        acc[...] += product
        mine, other = halves(keep_ref.shape[0])
        keep_ref[...] = acc[mine, :].astype(BF16)
        give_ref[...] = acc[other, :].astype(BF16)


def pair_kernel(keep_ref, come_ref, out_ref):
    out_ref[...] = (keep_ref[...].astype(F32) + come_ref[...].astype(F32)).astype(BF16)


def add_kernel(start, count, *refs):
    rows = refs[-1].shape[0]
    cut = slice(start, start + rows)
    total = sum(ref[cut].astype(F32) for ref in refs[:count])
    for ref in refs[count:-1]:
        total += ref[...].astype(F32)
    refs[-1][...] = total.astype(BF16)


def total_kernel(parts_ref, out_ref):
    total = parts_ref[0].astype(F32)
    for i in range(1, parts_ref.shape[0]):
        total += parts_ref[i].astype(F32)
    total = total.astype(BF16)
    for i in range(out_ref.shape[0]):
        out_ref[i] = total


def split(value):
    high = value.astype(BF16)
    return high, (value - high.astype(F32)).astype(BF16)


def joined(both):
    return both[:, :BLK].astype(F32) + both[:, BLK:].astype(F32)


def pair_gram_kernel(keep_ref, come_ref, out_ref):
    half = keep_ref.shape[0] // 2
    for i in range(out_ref.shape[0]):
        rows = slice(8 * i, 8 * i + 8)
        out_ref[i, :8] = (keep_ref[rows].astype(F32) + come_ref[rows].astype(F32)).astype(BF16)
        rows = slice(half + 8 * i, half + 8 * i + 8)
        out_ref[i, 8:, :BLK], out_ref[i, 8:, BLK:] = split(joined(keep_ref[rows]) + joined(come_ref[rows]))


def total_gram_kernel(parts_ref, out_ref):
    total = parts_ref[0].astype(F32)
    for i in range(1, parts_ref.shape[0]):
        total += parts_ref[i].astype(F32)
    rows = total[:8].astype(BF16)
    high, low = split(total[8:, :BLK] + total[8:, BLK:])
    for i in range(out_ref.shape[0]):
        out_ref[i, :8] = rows
        out_ref[i, 8:, :BLK] = high
        out_ref[i, 8:, BLK:] = low


def in_order(mine_ref, other_ref, out):
    for part, rows in zip((mine_ref, other_ref), halves(mine_ref.shape[0])):
        out[rows, :] = part[...]


def half_of(role):
    core = core_index()
    return role + core - 2 * role * core


def sample_kernel(ranks, full_ref, mine_ref, other_ref, *refs):
    outs, fwd = refs[:-1], refs[-1]
    in_order(mine_ref, other_ref, fwd)
    for rel in range(ranks):
        owner = lax.rem(lax.axis_index("obs") + rel, ranks)
        for half in range(2):
            outs[2 * rel + half][...] = dot_tn(full_ref[2 * owner + half_of(half)], fwd[...]).astype(BF16)


def pick_kernel(ranks, *refs):
    pieces, out_ref = refs[:-1], refs[-1]
    rel = lax.rem(core_index() * (ranks - 1) + ranks - lax.axis_index("obs"), ranks)
    for i in range(ranks):

        @pl.when(rel == i)
        def _():
            rows = pieces[2 * i].shape[0]
            out_ref[:rows] = pieces[2 * i][...]
            out_ref[rows:] = pieces[2 * i + 1][...]


def project_kernel(ranks, full_ref, *refs):
    pieces = refs[: 3 * ranks]
    sample_ref, keep_ref, give_ref, acc, gram = refs[3 * ranks :]
    rows = pieces[2].shape[0]
    total = jnp.zeros(acc.shape, F32)
    square = jnp.zeros(gram.shape, F32)
    for rel in range(ranks):
        owner = lax.rem(lax.axis_index("obs") + rel, ranks)
        for half in range(2):
            parts = pieces[3 * rel : 3 * rel + 2] if half == 0 else pieces[3 * rel + 2 : 3 * rel + 3]
            piece = jnp.concatenate([part[...] for part in parts], axis=0)
            chunk = 2 * owner + half_of(half)
            sample_ref[pl.ds(pl.multiple_of(chunk * rows, rows), rows), :] = piece
            total += dot(full_ref[chunk], piece)
            square += dot_tn(piece, piece)
    acc[...] = total
    gram[...] = square
    rows = acc.shape[0] // 2
    for out_ref, mine in zip((keep_ref, give_ref), halves(rows)):
        out_ref[:rows] = acc[mine, :].astype(BF16)
    for out_ref, mine in zip((keep_ref, give_ref), halves(BLK)):
        out_ref[rows : 2 * rows, :BLK], out_ref[rows : 2 * rows, BLK:] = split(gram[:, mine])
    core = core_index()
    last = sample_ref.shape[0] - EDGE
    give_ref[2 * rows :] = sample_ref[pl.ds(pl.multiple_of((1 - core) * last, EDGE), EDGE), :]


def prior_block(block, off_ref, coefs, ext, base):
    total = dot(coefs[0], ext[pl.ds(pl.multiple_of(base + block * BLK, BLK), BLK), :])
    for j in range(2):
        start = base + (block + off_ref[j, block]) * BLK
        total += dot(coefs[j + 1], ext[pl.ds(pl.multiple_of(start, BLK), BLK), :])
    return total.astype(BF16)


def fill_ends(sample_ref, come_ref, passed_ref, neighbor_ref, ext):
    rows = sample_ref.shape[0]
    core = core_index()
    ext[EDGE : 3 * EDGE] = sample_ref[: 2 * EDGE]
    ext[3 * EDGE : 5 * EDGE] = sample_ref[rows - 2 * EDGE :]
    ext[pl.ds(pl.multiple_of((1 - core) * (5 * EDGE), EDGE), EDGE)] = come_ref[come_ref.shape[0] - EDGE :]
    far = jnp.where(core == 0, passed_ref[...], neighbor_ref[...])
    ext[pl.ds(pl.multiple_of(core * (5 * EDGE), EDGE), EDGE)] = far


def packed(full):
    return jnp.concatenate(
        [
            full[:NB, : 2 * NB],
            full[:NB, 2 * NB :],
            full[NB : 2 * NB, NB : 3 * NB],
            full[2 * NB : 3 * NB, 2 * NB :],
            jnp.concatenate([full[NB : 2 * NB, 3 * NB :], full[3 * NB :, 3 * NB :]], axis=1),
        ],
        axis=0,
    )


def unpacked(pack):
    r = [pack[i * NB : (i + 1) * NB] for i in range(5)]
    zero = jnp.zeros((NB, NB), F32)
    lane = lax.broadcasted_iota(jnp.int32, (NB, 2 * NB), 1)
    head = lambda block: jnp.where(lane < NB, 0.5, 1.0) * block
    join = lambda *p: jnp.concatenate(p, axis=1)
    return jnp.concatenate(
        [
            join(head(r[0]), r[1]),
            join(zero, head(r[2]), r[4][:, :NB]),
            join(zero, zero, head(r[3])),
            join(zero, zero, zero, 0.5 * r[4][:, NB:]),
        ],
        axis=0,
    )


def moments_kernel(mine_ref, other_ref, gram_ref, second_ref, proj):
    count = mine_ref.shape[0]
    for part, core in ((mine_ref, core_index()), (other_ref, 1 - core_index())):
        columns = pl.ds(pl.multiple_of(core * BLK, BLK), BLK)
        for i in range(count):
            proj[pl.ds(pl.multiple_of(core * (8 * count) + 8 * i, 8), 8), :] = part[i, :8].astype(F32)
            gram_ref[8 * i : 8 * i + 8, columns] = joined(part[i, 8:])
    rounded = proj[...].astype(BF16)
    second_ref[...] = packed(dot_tn(rounded, rounded)).astype(BF16)


def row_of(tile, k):
    return jnp.broadcast_to(tile[k : k + 1, :], tile.shape)


def lane_of(tile, k):
    return jnp.broadcast_to(tile[:, k : k + 1], (8, 2 * NB))


def factor_inverse(block):
    index = [lax.broadcasted_iota(jnp.int32, (NB, NB), d) for d in (0, 1)]
    wide = jnp.concatenate([block, (index[0] == index[1]).astype(F32)], axis=1)
    groups = NB // 8
    tiles = [wide[8 * t : 8 * t + 8] for t in range(groups)]
    row = lax.broadcasted_iota(jnp.int32, (8, 2 * NB), 0)
    out = []
    for g in range(groups):
        cols = {t: [lane_of(tiles[t], 8 * g + k) for k in range(8)] for t in range(g, groups)}
        done = tiles[g]
        for k in range(0, 8, 2):
            here = cols[g]
            p, q, r = row_of(here[k], k), row_of(here[k + 1], k), row_of(here[k + 1], k + 1)
            root = lax.rsqrt(p * r - q * q)
            inverse = root * root
            p_root = lax.rsqrt(p)
            row0, row1 = row_of(tiles[g], k), row_of(tiles[g], k + 1)
            second = (p * p_root * root) * (row1 - (q * p_root * p_root) * row0)
            done = jnp.where(row == k, p_root * row0, jnp.where(row == k + 1, second, done))
            head0 = [row_of(here[j], k) for j in range(k + 2, 8)]
            head1 = [row_of(here[j], k + 1) for j in range(k + 2, 8)]
            for t in range(g, groups):
                c0, c1 = cols[t][k], cols[t][k + 1]
                w0 = r * c0 - q * c1
                w1 = p * c1 - q * c0
                for j in range(k + 2, 8):
                    cols[t][j] = cols[t][j] - inverse * (w0 * head0[j - k - 2] + w1 * head1[j - k - 2])
                change = inverse * (w0 * row0 + w1 * row1)
                if t == g:
                    change = jnp.where(row > k + 1, change, 0.0)
                tiles[t] = tiles[t] - change
        out.append(done)
    return jnp.concatenate(out, axis=0)[:, NB:]


def exact(a, b, nt=False):
    return dot_nt(a, b, HI) if nt else jnp.dot(a, b, precision=HI, preferred_element_type=F32)


def factor_kernel(
    scale, gram_ref, off_ref, coef_ref, sample_ref, come_ref, passed_ref, neighbor_ref, out_ref, image_ref, *scratch
):
    a_ref, m_ref, inv_ref, ext = scratch
    n = out_ref.shape[0]
    count, rows = coef_ref.shape[0], sample_ref.shape[0]
    share = count * NB // n
    fill_ends(sample_ref, come_ref, passed_ref, neighbor_ref, ext)
    gram = gram_ref[...] * scale
    index = [lax.broadcasted_iota(jnp.int32, (n, n), d) for d in (0, 1)]
    diagonal = jnp.where(index[0] == index[1], gram, 0.0)
    across = lax.rsqrt(jnp.sum(diagonal, axis=0, keepdims=True))
    a_ref[...] = gram * across * lax.rsqrt(jnp.sum(diagonal, axis=1, keepdims=True))
    m_ref[...] = jnp.zeros((n, n), F32)
    inv_ref[...] = jnp.zeros((n, n), F32)
    for lo in range(0, n, NB):
        hi, nx = lo + NB, lo + 2 * NB
        inverse = factor_inverse(a_ref[lo:hi, lo:hi])
        inv_ref[lo:hi, lo:hi] = inverse
        first = lo // NB * share
        for block in range(first, first + share):
            coefs = [coef_ref[block, j] for j in range(3)]
            source, base = sample_ref, 0
            if block < REACH:
                source, base = ext, EDGE
            elif block >= count - REACH:
                source, base = ext, 5 * EDGE - rows
            image_ref[block * BLK : (block + 1) * BLK] = prior_block(block, off_ref, coefs, source, base)
        if hi < n:
            upper = exact(inverse, a_ref[lo:hi, hi:])
            lower = exact(a_ref[hi:, lo:hi], inverse, nt=True)
            a_ref[hi:nx, hi:nx] -= exact(lower[:NB], upper[:, :NB])
            if nx < n:
                a_ref[hi:nx, nx:] -= exact(lower[:NB], upper[:, NB:])
                a_ref[nx:, hi:] -= exact(lower[NB:], upper)
        if lo:
            inv_ref[lo:hi, :lo] = exact(inverse, m_ref[lo:hi, :lo])
        if hi < n:
            m_ref[hi:, :hi] -= exact(lower, inv_ref[lo:hi, :hi])
    out_ref[...] = (inv_ref[...] * across).astype(BF16)


def final_kernel(scale, inv_ref, rows_ref, sample_ref, image_ref, *refs):
    seconds, (basis_ref, mapped_ref, ritz_ref) = refs[:-3], refs[-3:]
    inverse = inv_ref[...]
    basis_ref[...] = dot_nt(sample_ref[...], inverse).astype(BF16)
    mapped_ref[...] = dot_nt(image_ref[...], inverse).astype(BF16)
    total = seconds[0][...].astype(F32)
    for part in seconds[1:]:
        total += part[...].astype(F32)
    upper = unpacked(total).astype(BF16)
    left = dot(rows_ref[...], upper) + dot_nt(rows_ref[...], upper)
    ritz_ref[...] = dot_nt(left.astype(BF16), inverse) * scale


def shifted(value, axis, by):
    count = lax.axis_size(axis)
    return lax.ppermute(value, axis, [(i, (i + by) % count) for i in range(count)])


def to_neighbor(value):
    count = lax.axis_size("par")
    pairs = [pair for i in range(1, count - 1, 2) for pair in ((i, i + 1), (i + 1, i))]
    return lax.ppermute(value, "par", pairs)


def swapped(value):
    return lax.ppermute(value, "par", [(i, i ^ 1) for i in range(lax.axis_size("par"))])


def exchanged(parts):
    groups = [[2 * i + core for i in range(parts.shape[0])] for core in range(2)]
    return lax.all_to_all(parts, "par", 0, 0, axis_index_groups=groups, tiled=True)


def body(jacobian, probes, coeffs, offsets):
    ranks = lax.axis_size("obs")
    chips = lax.axis_size("par") // 2
    nobs, npar = jacobian.shape[0], jacobian.shape[1]
    width = probes.shape[1]
    count = coeffs.shape[0]
    offsets = offsets.T
    flops = 2 * nobs * npar * width

    whole = lambda *dims: pl.BlockSpec(dims, lambda i: (0,) * len(dims))
    chunks = npar // EDGE
    last = chunks - 1
    partner, neighbor = pl.pallas_call(
        functools.partial(edges_kernel, count),
        name="edges",
        grid=(2,),
        out_shape=[shape(nobs, EDGE)] * 2,
        in_specs=[
            SMEM,
            pl.BlockSpec((nobs, EDGE), lambda i: (0, i * last)),
            pl.BlockSpec((REACH, *coeffs.shape[1:]), lambda i: (i * last, 0, 0, 0)),
        ],
        out_specs=[whole(nobs, EDGE)] * 2,
        scratch_shapes=[pltpu.VMEM((REACH, nobs, BLK), F32)],
        compiler_params=pltpu.CompilerParams(vmem_limit_bytes=50 * 2**20),
        cost_estimate=pl.CostEstimate(flops=flops // 4, bytes_accessed=0, transcendentals=0),
    )(offsets, jacobian, coeffs)
    from_neighbor = to_neighbor(neighbor)
    from_partner = swapped(partner)
    own = call(
        own_kernel,
        shape(chunks, nobs, EDGE),
        [SMEM, VMEM, VMEM],
        [offsets, jacobian, coeffs],
        [pltpu.VMEM((count + 2 * REACH, nobs, BLK), F32)],
        flops=4 * flops,
    )
    half = shape(nobs // 2, width)
    inner = call(inner_kernel, shape(nobs, width, dtype=F32), [VMEM] * 2, [own, probes], flops=flops)
    edge_chunk = pl.BlockSpec((1, nobs, EDGE), lambda i: (i * last, 0, 0))
    full, keep, give = pl.pallas_call(
        forward_kernel,
        name="forward",
        grid=(2,),
        out_shape=[shape(chunks, nobs, EDGE), half, half],
        in_specs=[
            edge_chunk,
            whole(nobs, EDGE),
            whole(nobs, EDGE),
            pl.BlockSpec((EDGE, width), lambda i: (i * last, 0)),
            whole(nobs, width),
        ],
        out_specs=[edge_chunk, whole(*half.shape), whole(*half.shape)],
        scratch_shapes=[pltpu.VMEM((nobs, width), F32)],
        input_output_aliases={0: 0},
        compiler_params=pltpu.CompilerParams(vmem_limit_bytes=24 * 2**20),
    )(own, from_partner, from_neighbor, probes, inner)
    part = call(pair_kernel, half, [VMEM] * 2, [keep, swapped(give)], mib=4)
    parts = exchanged(part.reshape(chips, nobs // 2 // chips, width))
    total = call(total_kernel, shape(*parts.shape), [VMEM], [parts], mib=4)
    mine = exchanged(total).reshape(half.shape)
    other = swapped(mine)

    pieces = call(
        functools.partial(sample_kernel, ranks),
        [shape(npar // ranks // 2, width)] * (2 * ranks),
        [VMEM] * 3,
        [full, mine, other],
        [pltpu.VMEM((nobs, width), BF16)],
        mib=16,
        flops=flops,
    )
    here0, here1, right0, right1, far0, far1, left0, left1 = pieces

    def ring(value, by):
        return shifted(value, "obs", by)

    def add(start, rows, whole, parts=()):
        kernel = functools.partial(add_kernel, start, len(whole))
        return call(kernel, shape(rows, width), [VMEM] * (len(whole) + len(parts)), [*whole, *parts], mib=4)

    via_left = ring(far0, 1)
    via_right = ring(far1, -1)
    own_up = ring(right1, 1)
    own_down = ring(left0, -1)
    rows = EDGE // 2
    sums_up = [ring(add(i * rows, rows, [right0, via_left]), 1) for i in range(2)]
    sum_down = ring(add(0, EDGE, [left1, via_right]), -1)
    sums0 = [add(i * rows, rows, [here0, own_down], [sums_up[i]]) for i in range(2)]
    sum1 = add(0, EDGE, [here1, own_up, sum_down])
    l0 = [ring(sums0[i], 1) for i in range(2)]
    r0 = [ring(sums0[i], -1) for i in range(2)]
    f0 = [ring(l0[i], 1) for i in range(2)]
    l1 = ring(sum1, 1)
    r1 = ring(sum1, -1)
    f1 = ring(r1, -1)

    neighbor = call(
        functools.partial(pick_kernel, ranks), shape(EDGE, width), [VMEM] * (2 * ranks), [*sums0, *r0, *f0, *l0], mib=4
    )
    cores = lax.axis_size("par")
    passed = lax.ppermute(neighbor, "par", [(i, i + 2) for i in range(1, cores - 2, 2)])
    from_neighbor = lax.ppermute(neighbor, "par", [(i, i - 1) for i in range(2, cores, 2)])
    sample, keep, give = call(
        functools.partial(project_kernel, ranks),
        [shape(npar, width), shape(nobs, width), shape(nobs + EDGE, width)],
        [VMEM] * (1 + 3 * ranks),
        [full, *sums0, sum1, *r0, r1, *f0, f1, *l0, l1],
        [pltpu.VMEM((nobs, width), F32), pltpu.VMEM((width, width), F32)],
        mib=16,
        flops=flops,
    )
    come = swapped(give)
    both = shape(chips, 16, width)
    part = call(pair_gram_kernel, both, [VMEM] * 2, [keep, come], mib=4)
    total = call(total_gram_kernel, both, [VMEM], [exchanged(part)], mib=4)
    mine = exchanged(total)
    other = swapped(mine)
    passed = swapped(passed)
    gram, second = call(
        moments_kernel,
        [shape(width, width, dtype=F32), shape(5 * NB, 2 * NB)],
        [VMEM] * 2,
        [mine, other],
        [pltpu.VMEM((nobs, width), F32)],
        mib=8,
        flops=flops // 8,
    )
    seconds = [second] + [shifted(second, "obs", by) for by in (1, -1, 2)]
    total_par = npar * lax.axis_size("par")
    inverse, image = call(
        functools.partial(factor_kernel, 1.0 / total_par),
        [shape(width, width), shape(npar, width)],
        [VMEM, SMEM] + [VMEM] * 5,
        [gram, offsets, coeffs, sample, come, passed, from_neighbor],
        [pltpu.VMEM((width, width), F32)] * 3 + [pltpu.VMEM((6 * EDGE, width), BF16)],
        mib=16,
        flops=16 * flops,
    )
    steps = 2
    by_rows = pl.BlockSpec((npar // steps, width), lambda i: (i, 0))
    few = pl.BlockSpec((width // steps, width), lambda i: (i, 0))
    return pl.pallas_call(
        functools.partial(final_kernel, 1.0 / (nobs * ranks)),
        name="final",
        grid=(steps,),
        out_shape=[shape(npar, width), shape(npar, width), shape(width, width, dtype=F32)],
        in_specs=[whole(width, width), few, by_rows, by_rows] + [whole(*second.shape)] * len(seconds),
        out_specs=[by_rows, by_rows, few],
        compiler_params=pltpu.CompilerParams(vmem_limit_bytes=16 * 2**20),
    )(inverse, inverse, sample, image, *seconds)


def solution(mesh):
    return jax.shard_map(
        body,
        mesh=mesh,
        in_specs=(P("obs", "par"), P("par", None), P("par", None, None, None), P("par", None)),
        out_specs=(P("par", None), P("par", None), P()),
        check_vma=False,
    )
```
